128 devices in a mesh: gx: 8 (over x, core), yz: 16 (over z, y).
Axes of the slice: x: 4, y: 4, z: 4, core: 2. Of those that a mesh axis runs over, the one named last changes fastest.
Arguments:
- fine_blocks: bfloat16 [1024, 1536, 512], P(('gx', 'yz')), may hold values from -6 to 6
- fine_to_coarse: int32 [1024], replicated, may hold values from 0 to 511, as said below
- widths: int32 [1024], P(('gx', 'yz')), may hold values from 256 to 512
- pivots: int32 [512, 1024], P(('gx', 'yz')), may hold values from 0 to 1023, as said below
- neighbours: int32 [512, 4], P(('gx', 'yz')), may hold values from 0 to 3
Outputs:
- interp: float32 [512, 384, 640], P(('gx', 'yz'))
- schur_blocks: float32 [512, 384, 384], P(('gx', 'yz'))
The draws below stay inside these ranges and needn't reach their ends.
Inputs may be any that keep to these rules, and one draw needn't show every extreme that they name: `fine_to_coarse`: cluster c is owned by the device of index c // 4 along gx+yz, which has the same gx index as both its fine blocks; each cluster has exactly two fine blocks, on different devices, and the 8 blocks of one device belong to clusters of 8 different devices. `pivots`: each row is a permutation of 0 to 1023 whose first 384 entries are live columns (below the width of the first block, or 512 plus a column below the width of the second).
All inputs are finite; a program needn't handle non-finite values.
Results may differ from the reference program's by a relative error of at most 0.0003.
Values may be sent and summed in bfloat16 or wider, within the bound.
A program may use at most 192 MiB of HBM per device.

```python
import jax
import jax.numpy as jnp
from jax import lax

S = 512
K = 384
P_SIZE = 1536
FB_DEV = 8
NF = 1024
NC = 512
W = 1024
N_GX = 8
N_YZ = 16


def child_pairs_drawn(mapping):
    count = mapping.shape[0]
    ids = jnp.arange(count, dtype=jnp.int32)
    earlier = (mapping[None, :] == mapping[:, None]) & (ids[None, :] < ids[:, None])
    earlier_count = jnp.sum(earlier.astype(jnp.int32), axis=1).astype(jnp.int32)
    child_slot = (2 * mapping + earlier_count).astype(jnp.int32)
    children = jnp.zeros((count,), jnp.int32).at[child_slot].set(ids)
    return children.reshape(count // 2, 2)


def plan_group(group_key):
    split_keys = jax.random.split(group_key, 5)
    relabel = jax.random.permutation(split_keys[0], N_YZ).astype(jnp.int32)
    spread = jax.random.permutation(split_keys[1], N_YZ).astype(jnp.int32)
    offsets = jax.random.permutation(split_keys[2], N_YZ).astype(jnp.int32)[:FB_DEV]
    block_order = jax.vmap(lambda sub_key: jax.random.permutation(sub_key, FB_DEV))(jax.random.split(split_keys[3], N_YZ)).astype(jnp.int32)
    pairing = jax.vmap(lambda sub_key: jax.random.permutation(sub_key, FB_DEV))(jax.random.split(split_keys[4], N_YZ)).astype(jnp.int32)
    sources = jnp.arange(N_YZ, dtype=jnp.int32)[:, None]
    target = relabel[(spread[sources] + offsets[block_order]) % N_YZ]
    return (target * (FB_DEV // 2) + pairing[target, block_order] // 2).astype(jnp.int32)


def routing(key):
    plans = jax.vmap(plan_group)(jax.random.split(jax.random.fold_in(key, 7), N_GX))
    groups = jnp.arange(N_GX, dtype=jnp.int32)[:, None, None]
    mapping = (groups * (N_YZ * (FB_DEV // 2)) + plans).reshape(NF).astype(jnp.int32)
    fine_widths = jax.random.randint(jax.random.fold_in(key, 9), (NF,), S // 2, S + 1, dtype=jnp.int32)
    children = child_pairs_drawn(mapping)
    width_first = fine_widths[children[:, 0]][:, None]
    width_second = fine_widths[children[:, 1]][:, None]
    col_ids = jnp.arange(W, dtype=jnp.int32)[None, :]
    live_cols = jnp.where(col_ids < S, col_ids < width_first, col_ids - S < width_second)
    ranks = jax.vmap(lambda sub_key: jax.random.permutation(sub_key, W))(jax.random.split(jax.random.fold_in(key, 13), NC)).astype(jnp.int32)
    scores = ranks + jnp.where(live_cols, 0, W).astype(jnp.int32)
    order = jnp.argsort(scores, axis=1, stable=True).astype(jnp.int32)
    return (mapping, fine_widths, order)


def draw_fine_to_coarse(key, part):
    return routing(key)[0]


def draw_widths(key, part):
    return routing(key)[1]


def draw_pivots(key, part):
    return routing(key)[2]


def set_ends(result, rng, low, top_value):
    place = [jax.random.randint(jax.random.fold_in(rng, axis), (), 0, length) for axis, length in enumerate(result.shape)]
    widest = result.shape.index(max(result.shape))
    next_to = place[:widest] + [(place[widest] + 1) % result.shape[widest]] + place[widest + 1:]
    return result.at[tuple(place)].set(low).at[tuple(next_to)].set(top_value)


def levels(rng, shape, shards, low, high):
    factor_of, own = 1.0, jax.random.fold_in(rng, 6)
    for dim, blocks in shards:
        heights = jnp.exp(jax.random.uniform(jax.random.fold_in(own, dim), (blocks,), jnp.float32, low / len(shards), high / len(shards)))
        factor_of = factor_of * jnp.repeat(heights, shape[dim] // blocks).reshape([-1 if axis == dim else 1 for axis in range(len(shape))])
    return factor_of


def normal_values(stream_key, extent, scale, bound, shards=(), held_as=jnp.bfloat16):
    values = jax.random.normal(stream_key, extent, jnp.float32) * scale
    if len(shards) > 0:
        values = levels(stream_key, extent, shards, -0.22, 0.18) * values
    return jnp.clip(values, min=-bound, max=bound).astype(held_as)


def setup_inputs(seed: int = 0) -> dict:
    key_of = jax.random.split(jax.random.key(seed), 6)
    fine_blocks = normal_values(key_of[0], (NF, P_SIZE, S), 1.0, 6.0, ((0, 128),))
    fine_to_coarse = draw_fine_to_coarse(jax.random.fold_in(key_of[5], 71), 0)
    widths = draw_widths(jax.random.fold_in(key_of[5], 71), 0)
    pivots = draw_pivots(jax.random.fold_in(key_of[5], 71), 0)
    neighbours = set_ends(jax.random.randint(key_of[4], (NC, 4), 0, FB_DEV // 2), jax.random.fold_in(key_of[4], 1), 0, (FB_DEV // 2) - 1).astype(jnp.int32)
    return dict(fine_blocks=fine_blocks, fine_to_coarse=fine_to_coarse, widths=widths, pivots=pivots, neighbours=neighbours)


def child_pairs(mapping):
    count = mapping.shape[0]
    ids = jnp.arange(count, dtype=jnp.int32)
    earlier = (mapping[None, :] == mapping[:, None]) & (ids[None, :] < ids[:, None])
    earlier_count = jnp.sum(earlier.astype(jnp.int32), axis=1).astype(jnp.int32)
    child_slot = (2 * mapping + earlier_count).astype(jnp.int32)
    children = jnp.zeros((count,), jnp.int32).at[child_slot].set(ids)
    return children.reshape(count // 2, 2)

def reference(fine_blocks, fine_to_coarse, widths, pivots, neighbours):
    block_count = fine_blocks.shape[0]
    cluster_count = block_count // 2
    per_device = FB_DEV // 2
    column = jnp.arange(S, dtype=jnp.int32)
    live_cols = (column[None, :] < widths[:, None]).astype(jnp.bfloat16)
    masked = fine_blocks * live_cols[:, None, :]
    children = child_pairs(fine_to_coarse)

    def one_cluster(cluster):
        left_block = masked[children[cluster, 0]]
        right_block = masked[children[cluster, 1]]
        merged = jnp.concatenate([left_block, right_block], axis=1)
        pivoted = jnp.take(merged, pivots[cluster], axis=1)
        gram_rows = jnp.dot(pivoted[:, :K].T.astype(jnp.float32), pivoted.astype(jnp.float32), preferred_element_type=jnp.float32)
        factor = jnp.linalg.cholesky(gram_rows[:, :K])
        half_solved = jax.scipy.linalg.solve_triangular(factor, gram_rows[:, K:], lower=True)
        interp = jax.scipy.linalg.solve_triangular(factor, half_solved, lower=True, trans=1)
        update = jnp.dot(interp, interp.T, precision=lax.Precision.HIGHEST)
        return (interp, update)
    interp, update = lax.map(one_cluster, jnp.arange(cluster_count, dtype=jnp.int32))
    update_grid = update.reshape(N_GX, N_YZ, per_device, K, K)
    padded = jnp.pad(update_grid, ((1, 1), (1, 1), (0, 0), (0, 0), (0, 0)))

    def gather_one(cluster):
        gx_pos = cluster // (N_YZ * per_device)
        yz_pos = cluster // per_device % N_YZ
        chosen = neighbours[cluster]
        terms = padded[gx_pos, yz_pos + 1, chosen[0]] + padded[gx_pos + 2, yz_pos + 1, chosen[1]]
        terms = terms + padded[gx_pos + 1, yz_pos, chosen[2]] + padded[gx_pos + 1, yz_pos + 2, chosen[3]]
        return update[cluster] + terms
    schur_blocks = lax.map(gather_one, jnp.arange(cluster_count, dtype=jnp.int32))
    return (interp, schur_blocks)
```

```python
import functools

import jax
import jax.numpy as jnp
from jax import lax
from jax.experimental import pallas as pl
from jax.experimental.pallas import tpu as pltpu
from jax.sharding import PartitionSpec as P

K = 384
HIGH = lax.Precision.HIGHEST


def iota(shape, dim):
    return lax.broadcasted_iota(jnp.int32, shape, dim)


def place_kernel(target_ref, widths_ref, x_ref, o_ref):
    b = pl.program_id(0)
    x = x_ref[0]
    live = iota(x.shape, 1) < widths_ref[b]
    o_ref[0] = jnp.where(live, x, jnp.zeros_like(x))


def place_blocks(fine_blocks, target, widths, peers):
    count, rows, cols = fine_blocks.shape
    return pl.pallas_call(
        place_kernel,
        out_shape=jax.ShapeDtypeStruct((peers, rows, cols), fine_blocks.dtype),
        grid_spec=pltpu.PrefetchScalarGridSpec(
            num_scalar_prefetch=2,
            grid=(count,),
            in_specs=[pl.BlockSpec((1, rows, cols), lambda b, t, w: (b, 0, 0))],
            out_specs=pl.BlockSpec((1, rows, cols), lambda b, t, w: (t[b], 0, 0)),
        ),
        name="place_blocks",
    )(target, widths, fine_blocks)


def gram_kernel(first_ref, second_ref, a_ref, b_ref, piv_ref, o_ref, hot_ref):
    r = pl.program_id(1)
    half = a_ref.shape[2]

    @pl.when(r == 0)
    def _():
        hot_ref[...] = jnp.where(iota(hot_ref.shape, 0) == piv_ref[0], 1.0, 0.0).astype(hot_ref.dtype)

    pivoted = jnp.dot(a_ref[0], hot_ref[:half, :], preferred_element_type=jnp.float32)
    pivoted += jnp.dot(b_ref[0], hot_ref[half:, :], preferred_element_type=jnp.float32)
    pivoted = pivoted.astype(jnp.bfloat16)
    part = lax.dot_general(
        pivoted[:, :K], pivoted, (((0,), (0,)), ((), ())), preferred_element_type=jnp.float32
    )

    @pl.when(r == 0)
    def _():
        o_ref[0] = part

    @pl.when(r > 0)
    def _():
        o_ref[0] += part


def gram_of(arrived, first, second, pivots):
    peers, rows, half = arrived.shape
    clusters, width = pivots.shape
    step = 512
    return pl.pallas_call(
        gram_kernel,
        out_shape=jax.ShapeDtypeStruct((clusters, K, width), jnp.float32),
        grid_spec=pltpu.PrefetchScalarGridSpec(
            num_scalar_prefetch=2,
            grid=(clusters, rows // step),
            in_specs=[
                pl.BlockSpec((1, step, half), lambda c, r, f, s: (f[c], r, 0)),
                pl.BlockSpec((1, step, half), lambda c, r, f, s: (s[c], r, 0)),
                pl.BlockSpec((1, 1, width), lambda c, r, f, s: (c, 0, 0)),
            ],
            out_specs=pl.BlockSpec((1, K, width), lambda c, r, f, s: (c, 0, 0)),
            scratch_shapes=[pltpu.VMEM((width, width), jnp.bfloat16)],
        ),
        name="pivot_gram",
    )(first, second, arrived, arrived, pivots[:, None, :])


def packed_inverse(s):
    lane, row = iota(s.shape, 1), iota(s.shape, 0)
    inner = lane % 32
    base = lane - inner
    for k in range(32):
        col = jnp.take_along_axis(s, base + k, axis=1)
        here = inner == k
        scale = 1.0 / jnp.broadcast_to(col[k : k + 1], s.shape)
        scaled = jnp.where(here, scale, jnp.broadcast_to(s[k : k + 1], s.shape) * scale)
        s = jnp.where(row == k, scaled, jnp.where(here, 0.0, s) - col * scaled)
    return s


def invert_diagonal(d_ref):
    lane, row = iota((128, 128), 1), iota((128, 128), 0)
    lane32 = iota((32, 128), 1)
    for q in range(4):
        lo, hi = 32 * q, 32 * q + 32
        packed = jnp.zeros((32, 128), jnp.float32)
        for c in range(4):
            rows = d_ref[c, lo:hi, :]
            moved = pltpu.roll(rows, (32 * (c - q)) % 128, 1) if c != q else rows
            packed = jnp.where(lane32 // 32 == c, moved, packed)
        packed = packed_inverse(packed)
        in_cols = (lane >= lo) & (lane < hi)
        in_rows = (row >= lo) & (row < hi)
        in_lanes = (lane32 >= lo) & (lane32 < hi)
        for c in range(4):
            moved = pltpu.roll(packed, (32 * (q - c)) % 128, 1) if c != q else packed
            inverse = jnp.where(in_lanes, moved, 0.0)
            d = d_ref[c]
            scaled = jnp.dot(inverse, d, precision=HIGH, preferred_element_type=jnp.float32)
            scaled = jnp.where(in_lanes, inverse, scaled)
            parts = ([jnp.zeros((lo, 128), jnp.float32)] if lo else []) + [scaled]
            parts += [jnp.zeros((128 - hi, 128), jnp.float32)] if hi < 128 else []
            full = jnp.concatenate(parts, axis=0) if len(parts) > 1 else scaled
            lhs = jnp.where(in_cols & ~in_rows, -d, 0.0)
            kept = jnp.where(in_cols | in_rows, 0.0, d) + full
            d_ref[c] = kept + jnp.dot(lhs, full, precision=HIGH, preferred_element_type=jnp.float32)


def solve_kernel(g_ref, interp_ref, update_ref, w_ref, d_ref):
    clusters, width = g_ref.shape[0], g_ref.shape[2]
    w_ref[...] = g_ref[...]

    def eliminate(s, carry):
        at = pl.ds(pl.multiple_of(s * 128, 128), 128)
        for c in range(clusters):
            d_ref[c] = w_ref[c, at, at]
        invert_diagonal(d_ref)

        def one(c, carry):
            scaled = jnp.dot(d_ref[c], w_ref[c, at, :], precision=HIGH, preferred_element_type=jnp.float32)
            w_ref[c, at, :] = scaled
            for far in range(1, K // 128):
                other = lax.rem(s + far, K // 128)
                rows = pl.ds(pl.multiple_of(other * 128, 128), 128)
                w_ref[c, rows, :] = w_ref[c, rows, :] - jnp.dot(
                    w_ref[c, rows, at], scaled, precision=HIGH, preferred_element_type=jnp.float32
                )
            return carry

        return lax.fori_loop(0, clusters, one, carry)

    lax.fori_loop(0, K // 128, eliminate, 0)

    def finish(c, carry):
        x = w_ref[c, :, K:]
        interp_ref[c] = x
        update_ref[c] = lax.dot_general(
            x, x, (((1,), (1,)), ((), ())), precision=HIGH, preferred_element_type=jnp.float32
        )
        return carry

    lax.fori_loop(0, clusters, finish, 0)


def solve(gram):
    clusters, kept, width = gram.shape
    return pl.pallas_call(
        solve_kernel,
        out_shape=(
            jax.ShapeDtypeStruct((clusters, kept, width - kept), jnp.float32),
            jax.ShapeDtypeStruct((clusters, kept, kept), jnp.float32),
        ),
        in_specs=[pl.BlockSpec(memory_space=pltpu.VMEM)],
        out_specs=(pl.BlockSpec(memory_space=pltpu.VMEM), pl.BlockSpec(memory_space=pltpu.VMEM)),
        scratch_shapes=[
            pltpu.VMEM((clusters, kept, width), jnp.float32),
            pltpu.VMEM((clusters, 128, 128), jnp.float32),
        ],
        compiler_params=pltpu.CompilerParams(vmem_limit_bytes=56 * 1024 * 1024),
        name="solve_update",
    )(gram)


def schur_kernel(n_ref, own_ref, a_ref, b_ref, c_ref, d_ref, o_ref):
    o_ref[...] = own_ref[...] + ((a_ref[...] + b_ref[...]) + (c_ref[...] + d_ref[...]))


def gather_schur(update, sides, neighbours):
    clusters, kept, _ = update.shape

    def pick(side):
        return pl.BlockSpec((1, kept, kept), lambda c, n: (n[4 * c + side], 0, 0))

    own = pl.BlockSpec((1, kept, kept), lambda c, n: (c, 0, 0))
    return pl.pallas_call(
        schur_kernel,
        out_shape=jax.ShapeDtypeStruct(update.shape, jnp.float32),
        grid_spec=pltpu.PrefetchScalarGridSpec(
            num_scalar_prefetch=1,
            grid=(clusters,),
            in_specs=[own] + [pick(side) for side in range(4)],
            out_specs=own,
        ),
        name="gather_schur",
    )(neighbours.reshape(-1), update, *sides)


def from_sides(x):
    sides = []
    for axis in ("gx", "yz"):
        size = lax.axis_size(axis)
        up = [(i, i + 1) for i in range(size - 1)]
        sides += [lax.ppermute(x, axis, up), lax.ppermute(x, axis, [(b, a) for a, b in up])]
    return sides


def body(fine_blocks, fine_to_coarse, widths, pivots, neighbours):
    gx_count, yz_count = lax.axis_size("gx"), lax.axis_size("yz")
    gx_pos, yz_pos = lax.axis_index("gx"), lax.axis_index("yz")
    blocks_dev = fine_blocks.shape[0]
    clusters = blocks_dev // 2
    grouped = lax.dynamic_index_in_dim(
        fine_to_coarse.reshape(gx_count, yz_count, blocks_dev), gx_pos, 0, keepdims=False
    )
    owner, local = grouped // clusters - gx_pos * yz_count, grouped % clusters
    target = lax.dynamic_index_in_dim(owner, yz_pos, 0, keepdims=False)
    mine = (owner == yz_pos)[None] & (local[None] == jnp.arange(clusters, dtype=jnp.int32)[:, None, None])
    peer = jnp.arange(yz_count, dtype=jnp.int32)[None, :, None]
    first = jnp.min(jnp.where(mine, peer, yz_count - 1), axis=(1, 2))
    second = jnp.max(jnp.where(mine, peer, 0), axis=(1, 2))
    placed = place_blocks(fine_blocks, target, widths, yz_count)
    arrived = lax.all_to_all(placed, "yz", split_axis=0, concat_axis=0, tiled=True)
    interp, update = solve(gram_of(arrived, first, second, pivots))
    return interp, gather_schur(update, from_sides(update), neighbours)


def solution(mesh):
    split = ("gx", "yz")
    return jax.shard_map(
        body,
        mesh=mesh,
        in_specs=(P(split, None, None), P(), P(split), P(split, None), P(split, None)),
        out_specs=(P(split, None, None), P(split, None, None)),
        check_vma=False,
    )
```

```python
import functools

import jax
import jax.numpy as jnp
from jax import lax
from jax.experimental import pallas as pl
from jax.experimental.pallas import tpu as pltpu
from jax.sharding import PartitionSpec as P

K = 384
HIGH = lax.Precision.HIGHEST


def iota(shape, dim):
    return lax.broadcasted_iota(jnp.int32, shape, dim)


def place_kernel(target_ref, widths_ref, x_ref, o_ref):
    b = pl.program_id(0)
    x = x_ref[0]
    live = iota(x.shape, 1) < widths_ref[b]
    o_ref[0] = jnp.where(live, x, jnp.zeros_like(x))


def place_blocks(fine_blocks, target, widths, peers):
    count, rows, cols = fine_blocks.shape
    return pl.pallas_call(
        place_kernel,
        out_shape=jax.ShapeDtypeStruct((peers, rows, cols), fine_blocks.dtype),
        grid_spec=pltpu.PrefetchScalarGridSpec(
            num_scalar_prefetch=2,
            grid=(count,),
            in_specs=[pl.BlockSpec((1, rows, cols), lambda b, t, w: (b, 0, 0))],
            out_specs=pl.BlockSpec((1, rows, cols), lambda b, t, w: (t[b], 0, 0)),
        ),
        name="place_blocks",
    )(target, widths, fine_blocks)


GROUPS, PIECES = 6, 4


def exchange_gram_kernel(sel_ref, x_ref, piv_ref, o_ref, hot_ref, send_sem, recv_sems, own_sems, *lands):
    me = lax.axis_index("yz")
    plane = lax.axis_size("yz")
    side = 4
    clusters, kept, width = o_ref.shape
    peers, height, half = lands[0].shape
    step = height // PIECES

    def peer(d):
        return lax.rem(me // side + d // side, plane // side) * side + lax.rem(me + d, side)

    barrier = pltpu.get_barrier_semaphore()

    def greet(d, carry):
        pl.semaphore_signal(
            barrier, inc=1, device_id={"yz": peer(d)}, device_id_type=pl.DeviceIdType.MESH
        )
        return carry

    lax.fori_loop(1, peers, greet, 0)
    pl.semaphore_wait(barrier, peers - 1)

    def own_copy(group):
        rows = pl.ds(group * height, height)
        return pltpu.make_async_copy(x_ref.at[me, rows], lands[group].at[me], own_sems.at[group])

    def launch(group):
        def one(n, carry):
            piece, to = n // (peers - 1), peer(1 + lax.rem(n, peers - 1))
            pltpu.make_async_remote_copy(
                src_ref=x_ref.at[to, pl.ds(pl.multiple_of(group * height + piece * step, step), step)],
                dst_ref=lands[group].at[me, pl.ds(pl.multiple_of(piece * step, step), step)],
                send_sem=send_sem,
                recv_sem=recv_sems.at[group],
                device_id={"yz": to},
                device_id_type=pl.DeviceIdType.MESH,
            ).start()
            return carry

        lax.fori_loop(0, PIECES * (peers - 1), one, 0)
        own_copy(group).start()

    launch(0)
    launch(1)

    def make_hot(c, carry):
        hot_ref[c] = jnp.where(iota((width, width), 0) == piv_ref[c], 1.0, 0.0).astype(hot_ref.dtype)
        return carry

    lax.fori_loop(0, clusters, make_hot, 0)

    for group in range(GROUPS):
        land = lands[group]
        rest = land.at[pl.ds(0, peers - 1)]
        pltpu.make_async_copy(rest, rest, recv_sems.at[group]).wait()
        own_copy(group).wait()
        if group + 2 < GROUPS:
            launch(group + 2)

        def one_cluster(c, carry):
            a, b = land[sel_ref[0, c]], land[sel_ref[1, c]]
            pivoted = jnp.dot(a, hot_ref[c, :half, :], preferred_element_type=jnp.float32)
            pivoted += jnp.dot(b, hot_ref[c, half:, :], preferred_element_type=jnp.float32)
            pivoted = pivoted.astype(jnp.bfloat16)
            part = lax.dot_general(
                pivoted[:, :kept], pivoted, (((0,), (0,)), ((), ())), preferred_element_type=jnp.float32
            )
            o_ref[c] = part if group == 0 else o_ref[c] + part
            return carry

        lax.fori_loop(0, clusters, one_cluster, 0)

    whole = x_ref.at[pl.ds(0, peers - 1)]
    pltpu.make_async_copy(whole, whole, send_sem).wait()


def exchange_gram(placed, chosen, pivots):
    peers, rows, half = placed.shape
    clusters, width = pivots.shape
    height = rows // GROUPS
    vmem = pl.BlockSpec(memory_space=pltpu.VMEM)
    return pl.pallas_call(
        exchange_gram_kernel,
        out_shape=jax.ShapeDtypeStruct((clusters, K, width), jnp.float32),
        in_specs=[
            pl.BlockSpec(memory_space=pltpu.SMEM),
            pl.BlockSpec(memory_space=pltpu.HBM),
            vmem,
        ],
        out_specs=vmem,
        scratch_shapes=[
            pltpu.VMEM((clusters, width, width), jnp.bfloat16),
            pltpu.SemaphoreType.DMA,
            pltpu.SemaphoreType.DMA((GROUPS,)),
            pltpu.SemaphoreType.DMA((GROUPS,)),
        ]
        + [pltpu.VMEM((peers, height, half), jnp.bfloat16) for _ in range(GROUPS)],
        compiler_params=pltpu.CompilerParams(
            collective_id=0, has_side_effects=True, vmem_limit_bytes=58 * 1024 * 1024
        ),
        name="exchange_gram",
    )(chosen, placed, pivots[:, None, :])


def packed_inverse(s):
    lane, row = iota(s.shape, 1), iota(s.shape, 0)
    inner = lane % 32
    base = lane - inner
    for k in range(32):
        col = jnp.take_along_axis(s, base + k, axis=1)
        here = inner == k
        scale = 1.0 / jnp.broadcast_to(col[k : k + 1], s.shape)
        scaled = jnp.where(here, scale, jnp.broadcast_to(s[k : k + 1], s.shape) * scale)
        s = jnp.where(row == k, scaled, jnp.where(here, 0.0, s) - col * scaled)
    return s


def invert_diagonal(d_ref):
    lane, row = iota((128, 128), 1), iota((128, 128), 0)
    lane32 = iota((32, 128), 1)
    for q in range(4):
        lo, hi = 32 * q, 32 * q + 32
        packed = jnp.zeros((32, 128), jnp.float32)
        for c in range(4):
            rows = d_ref[c, lo:hi, :]
            moved = pltpu.roll(rows, (32 * (c - q)) % 128, 1) if c != q else rows
            packed = jnp.where(lane32 // 32 == c, moved, packed)
        packed = packed_inverse(packed)
        in_cols = (lane >= lo) & (lane < hi)
        in_rows = (row >= lo) & (row < hi)
        in_lanes = (lane32 >= lo) & (lane32 < hi)
        for c in range(4):
            moved = pltpu.roll(packed, (32 * (q - c)) % 128, 1) if c != q else packed
            inverse = jnp.where(in_lanes, moved, 0.0)
            d = d_ref[c]
            scaled = jnp.dot(inverse, d, precision=HIGH, preferred_element_type=jnp.float32)
            scaled = jnp.where(in_lanes, inverse, scaled)
            parts = ([jnp.zeros((lo, 128), jnp.float32)] if lo else []) + [scaled]
            parts += [jnp.zeros((128 - hi, 128), jnp.float32)] if hi < 128 else []
            full = jnp.concatenate(parts, axis=0) if len(parts) > 1 else scaled
            lhs = jnp.where(in_cols & ~in_rows, -d, 0.0)
            kept = jnp.where(in_cols | in_rows, 0.0, d) + full
            d_ref[c] = kept + jnp.dot(lhs, full, precision=HIGH, preferred_element_type=jnp.float32)


def solve_kernel(g_ref, interp_ref, update_ref, w_ref, d_ref):
    clusters, width = g_ref.shape[0], g_ref.shape[2]
    w_ref[...] = g_ref[...]

    def eliminate(s, carry):
        at = pl.ds(pl.multiple_of(s * 128, 128), 128)
        for c in range(clusters):
            d_ref[c] = w_ref[c, at, at]
        invert_diagonal(d_ref)

        def one(c, carry):
            scaled = jnp.dot(d_ref[c], w_ref[c, at, :], precision=HIGH, preferred_element_type=jnp.float32)
            w_ref[c, at, :] = scaled
            for far in range(1, K // 128):
                other = lax.rem(s + far, K // 128)
                rows = pl.ds(pl.multiple_of(other * 128, 128), 128)
                w_ref[c, rows, :] = w_ref[c, rows, :] - jnp.dot(
                    w_ref[c, rows, at], scaled, precision=HIGH, preferred_element_type=jnp.float32
                )
            return carry

        return lax.fori_loop(0, clusters, one, carry)

    lax.fori_loop(0, K // 128, eliminate, 0)

    def finish(c, carry):
        x = w_ref[c, :, K:]
        interp_ref[c] = x
        update_ref[c] = lax.dot_general(
            x, x, (((1,), (1,)), ((), ())), precision=HIGH, preferred_element_type=jnp.float32
        )
        return carry

    lax.fori_loop(0, clusters, finish, 0)


def solve(gram):
    clusters, kept, width = gram.shape
    return pl.pallas_call(
        solve_kernel,
        out_shape=(
            jax.ShapeDtypeStruct((clusters, kept, width - kept), jnp.float32),
            jax.ShapeDtypeStruct((clusters, kept, kept), jnp.float32),
        ),
        in_specs=[pl.BlockSpec(memory_space=pltpu.VMEM)],
        out_specs=(pl.BlockSpec(memory_space=pltpu.VMEM), pl.BlockSpec(memory_space=pltpu.VMEM)),
        scratch_shapes=[
            pltpu.VMEM((clusters, kept, width), jnp.float32),
            pltpu.VMEM((clusters, 128, 128), jnp.float32),
        ],
        compiler_params=pltpu.CompilerParams(vmem_limit_bytes=56 * 1024 * 1024),
        name="solve_update",
    )(gram)


def schur_kernel(n_ref, own_ref, a_ref, b_ref, c_ref, d_ref, o_ref):
    o_ref[...] = own_ref[...] + ((a_ref[...] + b_ref[...]) + (c_ref[...] + d_ref[...]))


def gather_schur(update, sides, neighbours):
    clusters, kept, _ = update.shape

    def pick(side):
        return pl.BlockSpec((1, kept, kept), lambda c, n: (n[4 * c + side], 0, 0))

    own = pl.BlockSpec((1, kept, kept), lambda c, n: (c, 0, 0))
    return pl.pallas_call(
        schur_kernel,
        out_shape=jax.ShapeDtypeStruct(update.shape, jnp.float32),
        grid_spec=pltpu.PrefetchScalarGridSpec(
            num_scalar_prefetch=1,
            grid=(clusters,),
            in_specs=[own] + [pick(side) for side in range(4)],
            out_specs=own,
        ),
        name="gather_schur",
    )(neighbours.reshape(-1), update, *sides)


def from_sides(x):
    sides = []
    for axis in ("gx", "yz"):
        size = lax.axis_size(axis)
        up = [(i, i + 1) for i in range(size - 1)]
        sides += [lax.ppermute(x, axis, up), lax.ppermute(x, axis, [(b, a) for a, b in up])]
    return sides


def body(fine_blocks, fine_to_coarse, widths, pivots, neighbours):
    gx_count, yz_count = lax.axis_size("gx"), lax.axis_size("yz")
    gx_pos, yz_pos = lax.axis_index("gx"), lax.axis_index("yz")
    blocks_dev = fine_blocks.shape[0]
    clusters = blocks_dev // 2
    grouped = lax.dynamic_index_in_dim(
        fine_to_coarse.reshape(gx_count, yz_count, blocks_dev), gx_pos, 0, keepdims=False
    )
    owner, local = grouped // clusters - gx_pos * yz_count, grouped % clusters
    target = lax.dynamic_index_in_dim(owner, yz_pos, 0, keepdims=False)
    mine = (owner == yz_pos)[None] & (local[None] == jnp.arange(clusters, dtype=jnp.int32)[:, None, None])
    peer = jnp.arange(yz_count, dtype=jnp.int32)[None, :, None]
    first = jnp.min(jnp.where(mine, peer, yz_count - 1), axis=(1, 2))
    second = jnp.max(jnp.where(mine, peer, 0), axis=(1, 2))
    placed = place_blocks(fine_blocks, target, widths, yz_count)
    interp, update = solve(exchange_gram(placed, jnp.stack([first, second]), pivots))
    return interp, gather_schur(update, from_sides(update), neighbours)


def solution(mesh):
    split = ("gx", "yz")
    return jax.shard_map(
        body,
        mesh=mesh,
        in_specs=(P(split, None, None), P(), P(split), P(split, None), P(split, None)),
        out_specs=(P(split, None, None), P(split, None, None)),
        check_vma=False,
    )
```

```python
import functools

import jax
import jax.numpy as jnp
from jax import lax
from jax.experimental import pallas as pl
from jax.experimental.pallas import tpu as pltpu
from jax.sharding import PartitionSpec as P

K = 384
HIGH = lax.Precision.HIGHEST


def iota(shape, dim):
    return lax.broadcasted_iota(jnp.int32, shape, dim)


def place_kernel(target_ref, widths_ref, x_ref, o_ref):
    b = pl.program_id(0)
    x = x_ref[0]
    live = iota(x.shape, 1) < widths_ref[b]
    o_ref[0] = jnp.where(live, x, jnp.zeros_like(x))


def place_blocks(fine_blocks, target, widths, peers):
    count, rows, cols = fine_blocks.shape
    return pl.pallas_call(
        place_kernel,
        out_shape=jax.ShapeDtypeStruct((peers, rows, cols), fine_blocks.dtype),
        grid_spec=pltpu.PrefetchScalarGridSpec(
            num_scalar_prefetch=2,
            grid=(count,),
            in_specs=[pl.BlockSpec((1, rows, cols), lambda b, t, w: (b, 0, 0))],
            out_specs=pl.BlockSpec((1, rows, cols), lambda b, t, w: (t[b], 0, 0)),
        ),
        name="place_blocks",
    )(target, widths, fine_blocks)


GROUPS, PIECES = 6, 4


def exchange_gram_kernel(sel_ref, x_ref, piv_ref, o_ref, hot_ref, send_sem, recv_sems, own_sems, *lands):
    me = lax.axis_index("yz")
    plane = lax.axis_size("yz")
    side = 4
    clusters, kept, width = o_ref.shape
    peers, height, half = lands[0].shape
    step = height // PIECES

    def peer(d):
        return lax.rem(me // side + d // side, plane // side) * side + lax.rem(me + d, side)

    barrier = pltpu.get_barrier_semaphore()

    def greet(d, carry):
        pl.semaphore_signal(
            barrier, inc=1, device_id={"yz": peer(d)}, device_id_type=pl.DeviceIdType.MESH
        )
        return carry

    lax.fori_loop(1, peers, greet, 0)
    pl.semaphore_wait(barrier, peers - 1)

    def own_copy(group):
        rows = pl.ds(group * height, height)
        return pltpu.make_async_copy(x_ref.at[me, rows], lands[group].at[me], own_sems.at[group])

    def launch(group):
        def one(n, carry):
            piece, to = n // (peers - 1), peer(1 + lax.rem(n, peers - 1))
            pltpu.make_async_remote_copy(
                src_ref=x_ref.at[to, pl.ds(pl.multiple_of(group * height + piece * step, step), step)],
                dst_ref=lands[group].at[me, pl.ds(pl.multiple_of(piece * step, step), step)],
                send_sem=send_sem,
                recv_sem=recv_sems.at[group],
                device_id={"yz": to},
                device_id_type=pl.DeviceIdType.MESH,
            ).start()
            return carry

        lax.fori_loop(0, PIECES * (peers - 1), one, 0)
        own_copy(group).start()

    launch(0)
    launch(1)

    def make_hot(c, carry):
        hot_ref[c] = jnp.where(iota((width, width), 0) == piv_ref[c], 1.0, 0.0).astype(hot_ref.dtype)
        return carry

    lax.fori_loop(0, clusters, make_hot, 0)

    for group in range(GROUPS):
        land = lands[group]
        rest = land.at[pl.ds(0, peers - 1)]
        pltpu.make_async_copy(rest, rest, recv_sems.at[group]).wait()
        own_copy(group).wait()
        if group + 2 < GROUPS:
            launch(group + 2)

        def one_cluster(c, carry):
            a, b = land[sel_ref[0, c]], land[sel_ref[1, c]]
            pivoted = jnp.dot(a, hot_ref[c, :half, :], preferred_element_type=jnp.float32)
            pivoted += jnp.dot(b, hot_ref[c, half:, :], preferred_element_type=jnp.float32)
            pivoted = pivoted.astype(jnp.bfloat16)
            part = lax.dot_general(
                pivoted[:, :kept], pivoted, (((0,), (0,)), ((), ())), preferred_element_type=jnp.float32
            )
            o_ref[c] = part if group == 0 else o_ref[c] + part
            return carry

        lax.fori_loop(0, clusters, one_cluster, 0)

    whole = x_ref.at[pl.ds(0, peers - 1)]
    pltpu.make_async_copy(whole, whole, send_sem).wait()


def exchange_gram(placed, chosen, pivots):
    peers, rows, half = placed.shape
    clusters, width = pivots.shape
    height = rows // GROUPS
    vmem = pl.BlockSpec(memory_space=pltpu.VMEM)
    return pl.pallas_call(
        exchange_gram_kernel,
        out_shape=jax.ShapeDtypeStruct((clusters, K, width), jnp.float32),
        in_specs=[
            pl.BlockSpec(memory_space=pltpu.SMEM),
            pl.BlockSpec(memory_space=pltpu.HBM),
            vmem,
        ],
        out_specs=vmem,
        scratch_shapes=[
            pltpu.VMEM((clusters, width, width), jnp.bfloat16),
            pltpu.SemaphoreType.DMA,
            pltpu.SemaphoreType.DMA((GROUPS,)),
            pltpu.SemaphoreType.DMA((GROUPS,)),
        ]
        + [pltpu.VMEM((peers, height, half), jnp.bfloat16) for _ in range(GROUPS)],
        compiler_params=pltpu.CompilerParams(
            collective_id=0, has_side_effects=True, vmem_limit_bytes=58 * 1024 * 1024
        ),
        name="exchange_gram",
    )(chosen, placed, pivots[:, None, :])


def packed_inverse(s):
    lane, row = iota((8, 128), 1), iota((8, 128), 0)
    inner = lane % 32
    base = lane - inner
    s = [s[8 * t : 8 * t + 8] for t in range(4)]

    def spread(x, k):
        return jnp.broadcast_to(x[k % 8 : k % 8 + 1], (8, 128))

    for k in range(0, 32, 4):
        at = k // 8
        cols = [
            [jnp.take_along_axis(x, base + (k + j), axis=1, mode="promise_in_bounds") for x in s]
            for j in range(4)
        ]
        here = (inner >= k) & (inner < k + 4)
        d = [[spread(cols[j][at], k + i) for j in range(4)] for i in range(4)]
        w = [jnp.where(here, jnp.where(inner == k + i, 1.0, 0.0), spread(s[at], k + i)) for i in range(4)]
        for p in range(4):
            scale = 1.0 / d[p][p]
            w[p] = w[p] * scale
            for j in range(p + 1, 4):
                d[p][j] = d[p][j] * scale
            for i in range(4):
                if i != p:
                    w[i] = w[i] - d[i][p] * w[p]
                    for j in range(p + 1, 4):
                        d[i][j] = d[i][j] - d[i][p] * d[p][j]
        for t in range(4):
            x = jnp.where(here, 0.0, s[t])
            x = x - (cols[0][t] * w[0] + cols[1][t] * w[1]) - (cols[2][t] * w[2] + cols[3][t] * w[3])
            if t == at:
                for i in range(4):
                    x = jnp.where(row == (k + i) % 8, w[i], x)
            s[t] = x
    return jnp.concatenate(s, axis=0)


def invert_diagonal(d_ref):
    lane, row = iota((128, 128), 1), iota((128, 128), 0)
    lane32 = iota((32, 128), 1)
    for q in range(4):
        lo, hi = 32 * q, 32 * q + 32
        packed = jnp.zeros((32, 128), jnp.float32)
        for c in range(4):
            rows = d_ref[c, lo:hi, :]
            moved = pltpu.roll(rows, (32 * (c - q)) % 128, 1) if c != q else rows
            packed = jnp.where(lane32 // 32 == c, moved, packed)
        packed = packed_inverse(packed)
        in_cols = (lane >= lo) & (lane < hi)
        in_rows = (row >= lo) & (row < hi)
        in_lanes = (lane32 >= lo) & (lane32 < hi)
        for c in range(4):
            moved = pltpu.roll(packed, (32 * (q - c)) % 128, 1) if c != q else packed
            inverse = jnp.where(in_lanes, moved, 0.0)
            d = d_ref[c]
            scaled = jnp.dot(inverse, d, precision=HIGH, preferred_element_type=jnp.float32)
            scaled = jnp.where(in_lanes, inverse, scaled)
            parts = ([jnp.zeros((lo, 128), jnp.float32)] if lo else []) + [scaled]
            parts += [jnp.zeros((128 - hi, 128), jnp.float32)] if hi < 128 else []
            full = jnp.concatenate(parts, axis=0) if len(parts) > 1 else scaled
            lhs = jnp.where(in_cols & ~in_rows, -d, 0.0)
            kept = jnp.where(in_cols | in_rows, 0.0, d) + full
            d_ref[c] = kept + jnp.dot(lhs, full, precision=HIGH, preferred_element_type=jnp.float32)


def split3(x):
    a = x.astype(jnp.bfloat16)
    x = x - a.astype(jnp.float32)
    b = x.astype(jnp.bfloat16)
    return a, b, (x - b.astype(jnp.float32)).astype(jnp.bfloat16)


def lhs_terms(x):
    a, b, c = split3(x)
    return jnp.concatenate([a, a, b, a, c, b], axis=1)


def rhs_terms(x):
    a, b, c = split3(x)
    return jnp.concatenate([a, b, a, c, a, b], axis=0)


LOWER = ((0, 0), (1, 0), (1, 1), (2, 0), (2, 1), (2, 2))


def solve_kernel(g_ref, interp_ref, update_ref, w_ref, d_ref):
    clusters, width = g_ref.shape[0], g_ref.shape[2]
    w_ref[...] = g_ref[...]

    def eliminate(s, carry):
        at = pl.ds(pl.multiple_of(s * 128, 128), 128)
        for c in range(clusters):
            d_ref[c] = w_ref[c, at, at]
        invert_diagonal(d_ref)

        def one(c, carry):
            scaled = jnp.dot(
                lhs_terms(d_ref[c]), rhs_terms(w_ref[c, at, :]), preferred_element_type=jnp.float32
            )
            w_ref[c, at, :] = scaled
            terms = rhs_terms(scaled)
            for far in range(1, K // 128):
                other = lax.rem(s + far, K // 128)
                rows = pl.ds(pl.multiple_of(other * 128, 128), 128)
                w_ref[c, rows, :] = w_ref[c, rows, :] - jnp.dot(
                    lhs_terms(w_ref[c, rows, at]), terms, preferred_element_type=jnp.float32
                )
            return carry

        return lax.fori_loop(0, clusters, one, carry)

    lax.fori_loop(0, K // 128, eliminate, 0)

    def finish(c, carry):
        x = w_ref[c, :, K:]
        interp_ref[c] = x
        a, b, _ = split3(x)
        lhs = jnp.concatenate([a, a, b], axis=1)
        rhs = jnp.concatenate([a, b, a], axis=1)
        across = (((1,), (1,)), ((), ()))
        left = lax.dot_general(lhs, rhs[:256], across, preferred_element_type=jnp.float32)
        last = lax.dot_general(lhs[256:], rhs[256:], across, preferred_element_type=jnp.float32)
        for n, (i, j) in enumerate(LOWER):
            update_ref[c, n] = last if j == 2 else left[128 * i : 128 * i + 128, 128 * j : 128 * j + 128]
        return carry

    lax.fori_loop(0, clusters, finish, 0)


def solve(gram):
    clusters, kept, width = gram.shape
    vmem = pl.BlockSpec(memory_space=pltpu.VMEM)
    return pl.pallas_call(
        solve_kernel,
        out_shape=(
            jax.ShapeDtypeStruct((clusters, kept, width - kept), jnp.float32),
            jax.ShapeDtypeStruct((clusters, len(LOWER), 128, 128), jnp.float32),
        ),
        in_specs=[vmem],
        out_specs=(vmem, vmem),
        scratch_shapes=[
            pltpu.VMEM((clusters, kept, width), jnp.float32),
            pltpu.VMEM((clusters, 128, 128), jnp.float32),
        ],
        compiler_params=pltpu.CompilerParams(vmem_limit_bytes=56 * 1024 * 1024),
        name="solve_update",
    )(gram)


def schur_kernel(n_ref, own_ref, a_ref, b_ref, c_ref, d_ref, o_ref):
    for n, (i, j) in enumerate(LOWER):
        x = own_ref[0, n] + ((a_ref[0, n] + b_ref[0, n]) + (c_ref[0, n] + d_ref[0, n]))
        o_ref[0, 128 * i : 128 * i + 128, 128 * j : 128 * j + 128] = x
        if i != j:
            o_ref[0, 128 * j : 128 * j + 128, 128 * i : 128 * i + 128] = x.T


def gather_schur(update, sides, neighbours):
    clusters = update.shape[0]
    block = (1,) + update.shape[1:]

    def pick(side):
        return pl.BlockSpec(block, lambda c, n: (n[4 * c + side], 0, 0, 0))

    return pl.pallas_call(
        schur_kernel,
        out_shape=jax.ShapeDtypeStruct((clusters, K, K), jnp.float32),
        grid_spec=pltpu.PrefetchScalarGridSpec(
            num_scalar_prefetch=1,
            grid=(clusters,),
            in_specs=[pl.BlockSpec(block, lambda c, n: (c, 0, 0, 0))] + [pick(side) for side in range(4)],
            out_specs=pl.BlockSpec((1, K, K), lambda c, n: (c, 0, 0)),
        ),
        name="gather_schur",
    )(neighbours.reshape(-1), update, *sides)


def from_sides(x):
    sides = []
    for axis in ("gx", "yz"):
        size = lax.axis_size(axis)
        up = [(i, i + 1) for i in range(size - 1)]
        sides += [lax.ppermute(x, axis, up), lax.ppermute(x, axis, [(b, a) for a, b in up])]
    return sides


def body(fine_blocks, fine_to_coarse, widths, pivots, neighbours):
    gx_count, yz_count = lax.axis_size("gx"), lax.axis_size("yz")
    gx_pos, yz_pos = lax.axis_index("gx"), lax.axis_index("yz")
    blocks_dev = fine_blocks.shape[0]
    clusters = blocks_dev // 2
    grouped = lax.dynamic_index_in_dim(
        fine_to_coarse.reshape(gx_count, yz_count, blocks_dev), gx_pos, 0, keepdims=False
    )
    owner, local = grouped // clusters - gx_pos * yz_count, grouped % clusters
    target = lax.dynamic_index_in_dim(owner, yz_pos, 0, keepdims=False)
    mine = (owner == yz_pos)[None] & (local[None] == jnp.arange(clusters, dtype=jnp.int32)[:, None, None])
    peer = jnp.arange(yz_count, dtype=jnp.int32)[None, :, None]
    first = jnp.min(jnp.where(mine, peer, yz_count - 1), axis=(1, 2))
    second = jnp.max(jnp.where(mine, peer, 0), axis=(1, 2))
    placed = place_blocks(fine_blocks, target, widths, yz_count)
    interp, update = solve(exchange_gram(placed, jnp.stack([first, second]), pivots))
    return interp, gather_schur(update, from_sides(update), neighbours)


def solution(mesh):
    split = ("gx", "yz")
    return jax.shard_map(
        body,
        mesh=mesh,
        in_specs=(P(split, None, None), P(), P(split), P(split, None), P(split, None)),
        out_specs=(P(split, None, None), P(split, None, None)),
        check_vma=False,
    )
```

```python
import functools

import jax
import jax.numpy as jnp
from jax import lax
from jax.experimental import pallas as pl
from jax.experimental.pallas import tpu as pltpu
from jax.sharding import PartitionSpec as P

K = 384
HIGH = lax.Precision.HIGHEST


def iota(shape, dim):
    return lax.broadcasted_iota(jnp.int32, shape, dim)


GROUPS, PIECES, STAGES = 6, 4, 3


def exchange_gram_kernel(
    sel_ref, slot_ref, x_ref, piv_ref, o_ref, hot_ref, send_sems, recv_sems, in_sems, *bufs
):
    lands, slots, blocks = bufs[:GROUPS], bufs[GROUPS : GROUPS + STAGES], bufs[GROUPS + STAGES :]
    me = lax.axis_index("yz")
    plane = lax.axis_size("yz")
    side = 4
    clusters, kept, width = o_ref.shape
    peers, height, half = lands[0].shape
    step = height // PIECES

    def peer(d):
        return lax.rem(me // side + d // side, plane // side) * side + lax.rem(me + d, side)

    def fetch(group):
        return pltpu.make_async_copy(
            x_ref.at[:, pl.ds(group * height, height)], blocks[group % 2], in_sems.at[group % 2]
        )

    fetch(0).start()
    fetch(1).start()
    barrier = pltpu.get_barrier_semaphore()

    def greet(d, carry):
        pl.semaphore_signal(
            barrier, inc=1, device_id={"yz": peer(d)}, device_id_type=pl.DeviceIdType.MESH
        )
        return carry

    lax.fori_loop(1, peers, greet, 0)

    def sent(group):
        rest = slots[group % STAGES].at[pl.ds(0, peers - 1)]
        pltpu.make_async_copy(rest, rest, send_sems.at[group % STAGES]).wait()

    def fill(group):
        fetch(group).wait()
        if group >= STAGES:
            sent(group - STAGES)
        column = iota((height, half), 1)

        def masked(t):
            x = blocks[group % 2][slot_ref[0, t]]
            return jnp.where(column < slot_ref[1, t], x, jnp.zeros_like(x))

        def one(d, carry):
            slots[group % STAGES][peer(d)] = masked(peer(d))
            return carry

        lax.fori_loop(1, peers, one, 0)
        lands[group][me] = masked(me)
        if group + 2 < GROUPS:
            fetch(group + 2).start()

    def launch(group):
        def one(n, carry):
            piece, to = n // (peers - 1), peer(1 + lax.rem(n, peers - 1))
            rows = pl.ds(pl.multiple_of(piece * step, step), step)
            pltpu.make_async_remote_copy(
                src_ref=slots[group % STAGES].at[to, rows],
                dst_ref=lands[group].at[me, rows],
                send_sem=send_sems.at[group % STAGES],
                recv_sem=recv_sems.at[group],
                device_id={"yz": to},
                device_id_type=pl.DeviceIdType.MESH,
            ).start()
            return carry

        lax.fori_loop(0, PIECES * (peers - 1), one, 0)

    fill(0)
    pl.semaphore_wait(barrier, peers - 1)
    launch(0)
    fill(1)
    launch(1)

    def make_hot(c, carry):
        hot_ref[c] = jnp.where(iota((width, width), 0) == piv_ref[c], 1.0, 0.0).astype(hot_ref.dtype)
        return carry

    lax.fori_loop(0, clusters, make_hot, 0)
    fill(2)

    for group in range(GROUPS):
        land = lands[group]
        rest = land.at[pl.ds(0, peers - 1)]
        pltpu.make_async_copy(rest, rest, recv_sems.at[group]).wait()
        if group + 2 < GROUPS:
            launch(group + 2)

        def one_cluster(c, carry):
            a, b = land[sel_ref[0, c]], land[sel_ref[1, c]]
            pivoted = jnp.dot(a, hot_ref[c, :half, :], preferred_element_type=jnp.float32)
            pivoted += jnp.dot(b, hot_ref[c, half:, :], preferred_element_type=jnp.float32)
            pivoted = pivoted.astype(jnp.bfloat16)
            part = lax.dot_general(
                pivoted[:, :kept], pivoted, (((0,), (0,)), ((), ())), preferred_element_type=jnp.float32
            )
            o_ref[c] = part if group == 0 else o_ref[c] + part
            return carry

        lax.fori_loop(0, clusters, one_cluster, 0)
        if group + STAGES < GROUPS:
            fill(group + STAGES)

    for group in range(GROUPS - STAGES, GROUPS):
        sent(group)


def exchange_gram(fine_blocks, slots, chosen, pivots):
    count, rows, half = fine_blocks.shape
    peers = slots.shape[1]
    clusters, width = pivots.shape
    height = rows // GROUPS
    vmem, smem = pl.BlockSpec(memory_space=pltpu.VMEM), pl.BlockSpec(memory_space=pltpu.SMEM)
    return pl.pallas_call(
        exchange_gram_kernel,
        out_shape=jax.ShapeDtypeStruct((clusters, K, width), jnp.float32),
        in_specs=[smem, smem, pl.BlockSpec(memory_space=pltpu.HBM), vmem],
        out_specs=vmem,
        scratch_shapes=[
            pltpu.VMEM((clusters, width, width), jnp.bfloat16),
            pltpu.SemaphoreType.DMA((STAGES,)),
            pltpu.SemaphoreType.DMA((GROUPS,)),
            pltpu.SemaphoreType.DMA((2,)),
        ]
        + [pltpu.VMEM((peers, height, half), jnp.bfloat16) for _ in range(GROUPS + STAGES)]
        + [pltpu.VMEM((count, height, half), jnp.bfloat16) for _ in range(2)],
        compiler_params=pltpu.CompilerParams(
            collective_id=0, has_side_effects=True, vmem_limit_bytes=63 * 1024 * 1024
        ),
        name="exchange_gram",
    )(chosen, slots, fine_blocks, pivots[:, None, :])


def packed_inverse(s):
    lane, row = iota((8, 128), 1), iota((8, 128), 0)
    inner = lane % 32
    base = lane - inner
    s = [s[8 * t : 8 * t + 8] for t in range(4)]

    def spread(x, k):
        return jnp.broadcast_to(x[k % 8 : k % 8 + 1], (8, 128))

    for k in range(0, 32, 4):
        at = k // 8
        cols = [
            [jnp.take_along_axis(x, base + (k + j), axis=1, mode="promise_in_bounds") for x in s]
            for j in range(4)
        ]
        here = (inner >= k) & (inner < k + 4)
        d = [[spread(cols[j][at], k + i) for j in range(4)] for i in range(4)]
        w = [jnp.where(here, jnp.where(inner == k + i, 1.0, 0.0), spread(s[at], k + i)) for i in range(4)]
        for p in range(4):
            scale = 1.0 / d[p][p]
            w[p] = w[p] * scale
            for j in range(p + 1, 4):
                d[p][j] = d[p][j] * scale
            for i in range(4):
                if i != p:
                    w[i] = w[i] - d[i][p] * w[p]
                    for j in range(p + 1, 4):
                        d[i][j] = d[i][j] - d[i][p] * d[p][j]
        for t in range(4):
            x = jnp.where(here, 0.0, s[t])
            x = x - (cols[0][t] * w[0] + cols[1][t] * w[1]) - (cols[2][t] * w[2] + cols[3][t] * w[3])
            if t == at:
                for i in range(4):
                    x = jnp.where(row == (k + i) % 8, w[i], x)
            s[t] = x
    return jnp.concatenate(s, axis=0)


def split3(x):
    a = x.astype(jnp.bfloat16)
    x = x - a.astype(jnp.float32)
    b = x.astype(jnp.bfloat16)
    return a, b, (x - b.astype(jnp.float32)).astype(jnp.bfloat16)


def lhs_terms(x):
    a, b, c = split3(x)
    return jnp.concatenate([a, a, b, a, c, b], axis=1)


def rhs_terms(x):
    a, b, c = split3(x)
    return jnp.concatenate([a, b, a, c, a, b], axis=0)


def invert_diagonal(d_ref):
    lane = iota((128, 128), 1)
    lane32 = iota((32, 128), 1)
    segment = lane32 // 32
    pad = jnp.zeros((64, 128), jnp.bfloat16)
    for q in range(4):
        lo, hi = 32 * q, 32 * q + 32
        packed = jnp.zeros((32, 128), jnp.float32)
        for c in range(4):
            rows = d_ref[c, lo:hi, :]
            moved = pltpu.roll(rows, (32 * (c - q)) % 128, 1) if c != q else rows
            packed = jnp.where(segment == c, moved, packed)
        packed = packed_inverse(packed)
        turned = [packed] + [pltpu.roll(packed, 32 * t, 1) for t in range(1, 4)]
        in_cols = (lane >= lo) & (lane < hi)
        in_lanes = segment == q
        for c in range(4):
            inverse = turned[(0 - c) % 4]
            for t in range(1, 4):
                inverse = jnp.where(segment == t, turned[(t - c) % 4], inverse)
            a, b, e = split3(inverse)
            none = jnp.zeros_like(a)
            lhs = jnp.concatenate(
                [
                    jnp.where(segment == 2, b, a),
                    jnp.where(segment == 0, e, jnp.where(segment == 1, b, none)),
                ],
                axis=1,
            )
            rows = d_ref[c, lo:hi, :]
            rhs = jnp.concatenate([rhs_terms(rows), pad], axis=0)
            scaled = jnp.dot(lhs, rhs, preferred_element_type=jnp.float32)
            scaled = jnp.where(in_lanes, inverse, scaled)
            a, b, e = split3(jnp.where(in_lanes, 0.0, jnp.where(lane32 < lo, rows, -rows)))
            lhs = jnp.concatenate([a, a, b, a, e, b, pad], axis=0)
            rhs = jnp.concatenate([rhs_terms(scaled), pad], axis=0)
            change = lax.dot_general(
                lhs, rhs, (((0,), (0,)), ((), ())), preferred_element_type=jnp.float32
            )
            d_ref[c] = jnp.where(in_cols, 0.0, d_ref[c]) + change
            d_ref[c, lo:hi, :] = scaled


LOWER = ((0, 0), (1, 0), (1, 1), (2, 0), (2, 1), (2, 2))


def solve_kernel(g_ref, interp_ref, update_ref, w_ref, d_ref):
    clusters, width = g_ref.shape[0], g_ref.shape[2]
    w_ref[...] = g_ref[...]

    def eliminate(s, carry):
        at = pl.ds(pl.multiple_of(s * 128, 128), 128)
        for c in range(clusters):
            d_ref[c] = w_ref[c, at, at]
        invert_diagonal(d_ref)

        def one(c, carry):
            scaled = jnp.dot(
                lhs_terms(d_ref[c]), rhs_terms(w_ref[c, at, :]), preferred_element_type=jnp.float32
            )
            w_ref[c, at, :] = scaled
            terms = rhs_terms(scaled)
            for far in range(1, K // 128):
                other = lax.rem(s + far, K // 128)
                rows = pl.ds(pl.multiple_of(other * 128, 128), 128)
                w_ref[c, rows, :] = w_ref[c, rows, :] - jnp.dot(
                    lhs_terms(w_ref[c, rows, at]), terms, preferred_element_type=jnp.float32
                )
            return carry

        return lax.fori_loop(0, clusters, one, carry)

    lax.fori_loop(0, K // 128, eliminate, 0)

    def finish(c, carry):
        x = w_ref[c, :, K:]
        interp_ref[c] = x
        a, b, _ = split3(x)
        lhs = jnp.concatenate([a, a, b], axis=1)
        rhs = jnp.concatenate([a, b, a], axis=1)
        across = (((1,), (1,)), ((), ()))
        left = lax.dot_general(lhs, rhs[:256], across, preferred_element_type=jnp.float32)
        last = lax.dot_general(lhs[256:], rhs[256:], across, preferred_element_type=jnp.float32)
        for n, (i, j) in enumerate(LOWER):
            update_ref[c, n] = last if j == 2 else left[128 * i : 128 * i + 128, 128 * j : 128 * j + 128]
        return carry

    lax.fori_loop(0, clusters, finish, 0)


def solve(gram):
    clusters, kept, width = gram.shape
    vmem = pl.BlockSpec(memory_space=pltpu.VMEM)
    return pl.pallas_call(
        solve_kernel,
        out_shape=(
            jax.ShapeDtypeStruct((clusters, kept, width - kept), jnp.float32),
            jax.ShapeDtypeStruct((clusters, len(LOWER), 128, 128), jnp.float32),
        ),
        in_specs=[vmem],
        out_specs=(vmem, vmem),
        scratch_shapes=[
            pltpu.VMEM((clusters, kept, width), jnp.float32),
            pltpu.VMEM((clusters, 128, 128), jnp.float32),
        ],
        compiler_params=pltpu.CompilerParams(vmem_limit_bytes=56 * 1024 * 1024),
        name="solve_update",
    )(gram)


def schur_kernel(n_ref, own_ref, a_ref, b_ref, c_ref, d_ref, o_ref):
    for n, (i, j) in enumerate(LOWER):
        x = own_ref[0, n] + ((a_ref[0, n] + b_ref[0, n]) + (c_ref[0, n] + d_ref[0, n]))
        o_ref[0, 128 * i : 128 * i + 128, 128 * j : 128 * j + 128] = x
        if i != j:
            o_ref[0, 128 * j : 128 * j + 128, 128 * i : 128 * i + 128] = x.T


def gather_schur(update, sides, neighbours):
    clusters = update.shape[0]
    block = (1,) + update.shape[1:]

    def pick(side):
        return pl.BlockSpec(block, lambda c, n: (n[4 * c + side], 0, 0, 0))

    return pl.pallas_call(
        schur_kernel,
        out_shape=jax.ShapeDtypeStruct((clusters, K, K), jnp.float32),
        grid_spec=pltpu.PrefetchScalarGridSpec(
            num_scalar_prefetch=1,
            grid=(clusters,),
            in_specs=[pl.BlockSpec(block, lambda c, n: (c, 0, 0, 0))] + [pick(side) for side in range(4)],
            out_specs=pl.BlockSpec((1, K, K), lambda c, n: (c, 0, 0)),
        ),
        name="gather_schur",
    )(neighbours.reshape(-1), update, *sides)


def from_sides(x):
    sides = []
    for axis in ("gx", "yz"):
        size = lax.axis_size(axis)
        up = [(i, i + 1) for i in range(size - 1)]
        sides += [lax.ppermute(x, axis, up), lax.ppermute(x, axis, [(b, a) for a, b in up])]
    return sides


def body(fine_blocks, fine_to_coarse, widths, pivots, neighbours):
    gx_count, yz_count = lax.axis_size("gx"), lax.axis_size("yz")
    gx_pos, yz_pos = lax.axis_index("gx"), lax.axis_index("yz")
    blocks_dev = fine_blocks.shape[0]
    clusters = blocks_dev // 2
    grouped = lax.dynamic_index_in_dim(
        fine_to_coarse.reshape(gx_count, yz_count, blocks_dev), gx_pos, 0, keepdims=False
    )
    owner, local = grouped // clusters - gx_pos * yz_count, grouped % clusters
    target = lax.dynamic_index_in_dim(owner, yz_pos, 0, keepdims=False)
    mine = (owner == yz_pos)[None] & (local[None] == jnp.arange(clusters, dtype=jnp.int32)[:, None, None])
    peer = jnp.arange(yz_count, dtype=jnp.int32)[None, :, None]
    first = jnp.min(jnp.where(mine, peer, yz_count - 1), axis=(1, 2))
    second = jnp.max(jnp.where(mine, peer, 0), axis=(1, 2))
    goes = target[None, :] == jnp.arange(yz_count, dtype=jnp.int32)[:, None]
    numbers = jnp.stack([jnp.arange(blocks_dev, dtype=jnp.int32), widths])
    slots = jnp.sum(jnp.where(goes[None], numbers[:, None, :], 0), axis=2)
    interp, update = solve(exchange_gram(fine_blocks, slots, jnp.stack([first, second]), pivots))
    return interp, gather_schur(update, from_sides(update), neighbours)


def solution(mesh):
    split = ("gx", "yz")
    return jax.shard_map(
        body,
        mesh=mesh,
        in_specs=(P(split, None, None), P(), P(split), P(split, None), P(split, None)),
        out_specs=(P(split, None, None), P(split, None, None)),
        check_vma=False,
    )
```

```python
import functools

import jax
import jax.numpy as jnp
from jax import lax
from jax.experimental import pallas as pl
from jax.experimental.pallas import tpu as pltpu
from jax.sharding import PartitionSpec as P

K = 384
HIGH = lax.Precision.HIGHEST


def iota(shape, dim):
    return lax.broadcasted_iota(jnp.int32, shape, dim)


GROUPS, PIECES, STAGES = 6, 4, 3


def exchange_gram_kernel(
    sel_ref, slot_ref, x_ref, piv_ref, o_ref, hot_ref, send_sems, recv_sems, in_sems, *bufs
):
    lands, slots, blocks = bufs[:GROUPS], bufs[GROUPS : GROUPS + STAGES], bufs[GROUPS + STAGES :]
    me = lax.axis_index("yz")
    plane = lax.axis_size("yz")
    side = 4
    clusters, kept, width = o_ref.shape
    peers, height, half = lands[0].shape
    step = height // PIECES

    def peer(d):
        return lax.rem(me // side + d // side, plane // side) * side + lax.rem(me + d, side)

    def fetch(group):
        return pltpu.make_async_copy(
            x_ref.at[:, pl.ds(group * height, height)], blocks[group % 2], in_sems.at[group % 2]
        )

    fetch(0).start()
    fetch(1).start()
    barrier = pltpu.get_barrier_semaphore()

    def greet(d, carry):
        pl.semaphore_signal(
            barrier, inc=1, device_id={"yz": peer(d)}, device_id_type=pl.DeviceIdType.MESH
        )
        return carry

    lax.fori_loop(1, peers, greet, 0)

    def sent(group):
        rest = slots[group % STAGES].at[pl.ds(0, peers - 1)]
        pltpu.make_async_copy(rest, rest, send_sems.at[group % STAGES]).wait()

    def fill(group):
        fetch(group).wait()
        if group >= STAGES:
            sent(group - STAGES)
        column = iota((height, half), 1)

        def masked(t):
            x = blocks[group % 2][slot_ref[0, t]]
            return jnp.where(column < slot_ref[1, t], x, jnp.zeros_like(x))

        def one(d, carry):
            slots[group % STAGES][peer(d)] = masked(peer(d))
            return carry

        lax.fori_loop(1, peers, one, 0)
        lands[group][me] = masked(me)
        if group + 2 < GROUPS:
            fetch(group + 2).start()

    def launch(group):
        def one(n, carry):
            piece, to = n // (peers - 1), peer(1 + lax.rem(n, peers - 1))
            rows = pl.ds(pl.multiple_of(piece * step, step), step)
            pltpu.make_async_remote_copy(
                src_ref=slots[group % STAGES].at[to, rows],
                dst_ref=lands[group].at[me, rows],
                send_sem=send_sems.at[group % STAGES],
                recv_sem=recv_sems.at[group],
                device_id={"yz": to},
                device_id_type=pl.DeviceIdType.MESH,
            ).start()
            return carry

        lax.fori_loop(0, PIECES * (peers - 1), one, 0)

    fill(0)
    pl.semaphore_wait(barrier, peers - 1)
    launch(0)
    fill(1)
    launch(1)

    def make_hot(c, carry):
        hot_ref[c] = jnp.where(iota((width, width), 0) == piv_ref[pl.ds(c, 1), :], 1.0, 0.0).astype(hot_ref.dtype)
        return carry

    lax.fori_loop(0, clusters, make_hot, 0)
    fill(2)

    for group in range(GROUPS):
        land = lands[group]
        rest = land.at[pl.ds(0, peers - 1)]
        pltpu.make_async_copy(rest, rest, recv_sems.at[group]).wait()
        if group + 2 < GROUPS:
            launch(group + 2)

        def one_cluster(c, carry):
            a, b = land[sel_ref[0, c]], land[sel_ref[1, c]]
            pivoted = jnp.dot(a, hot_ref[c, :half, :], preferred_element_type=jnp.float32)
            pivoted += jnp.dot(b, hot_ref[c, half:, :], preferred_element_type=jnp.float32)
            pivoted = pivoted.astype(jnp.bfloat16)
            part = lax.dot_general(
                pivoted[:, :kept], pivoted, (((0,), (0,)), ((), ())), preferred_element_type=jnp.float32
            )
            o_ref[c] = part if group == 0 else o_ref[c] + part
            return carry

        lax.fori_loop(0, clusters, one_cluster, 0)
        if group + STAGES < GROUPS:
            fill(group + STAGES)

    for group in range(GROUPS - STAGES, GROUPS):
        sent(group)


def exchange_gram(fine_blocks, slots, chosen, pivots):
    count, rows, half = fine_blocks.shape
    peers = slots.shape[1]
    clusters, width = pivots.shape
    height = rows // GROUPS
    vmem, smem = pl.BlockSpec(memory_space=pltpu.VMEM), pl.BlockSpec(memory_space=pltpu.SMEM)
    return pl.pallas_call(
        exchange_gram_kernel,
        out_shape=jax.ShapeDtypeStruct((clusters, K, width), jnp.float32),
        in_specs=[smem, smem, pl.BlockSpec(memory_space=pltpu.HBM), vmem],
        out_specs=vmem,
        scratch_shapes=[
            pltpu.VMEM((clusters, width, width), jnp.bfloat16),
            pltpu.SemaphoreType.DMA((STAGES,)),
            pltpu.SemaphoreType.DMA((GROUPS,)),
            pltpu.SemaphoreType.DMA((2,)),
        ]
        + [pltpu.VMEM((peers, height, half), jnp.bfloat16) for _ in range(GROUPS + STAGES)]
        + [pltpu.VMEM((count, height, half), jnp.bfloat16) for _ in range(2)],
        compiler_params=pltpu.CompilerParams(
            collective_id=0, has_side_effects=True, vmem_limit_bytes=63 * 1024 * 1024
        ),
        name="exchange_gram",
    )(chosen, slots, fine_blocks, pivots)


def packed_inverse(s):
    lane, row = iota((8, 128), 1), iota((8, 128), 0)
    inner = lane % 32
    base = lane - inner
    s = [s[8 * t : 8 * t + 8] for t in range(4)]

    def spread(x, k):
        return jnp.broadcast_to(x[k % 8 : k % 8 + 1], (8, 128))

    for k in range(0, 32, 4):
        at = k // 8
        cols = [
            [jnp.take_along_axis(x, base + (k + j), axis=1, mode="promise_in_bounds") for x in s]
            for j in range(4)
        ]
        here = (inner >= k) & (inner < k + 4)
        d = [[spread(cols[j][at], k + i) for j in range(4)] for i in range(4)]
        w = [jnp.where(here, jnp.where(inner == k + i, 1.0, 0.0), spread(s[at], k + i)) for i in range(4)]
        for p in range(4):
            scale = 1.0 / d[p][p]
            w[p] = w[p] * scale
            for j in range(p + 1, 4):
                d[p][j] = d[p][j] * scale
            for i in range(4):
                if i != p:
                    w[i] = w[i] - d[i][p] * w[p]
                    for j in range(p + 1, 4):
                        d[i][j] = d[i][j] - d[i][p] * d[p][j]
        for t in range(4):
            x = jnp.where(here, 0.0, s[t])
            x = x - (cols[0][t] * w[0] + cols[1][t] * w[1]) - (cols[2][t] * w[2] + cols[3][t] * w[3])
            if t == at:
                for i in range(4):
                    x = jnp.where(row == (k + i) % 8, w[i], x)
            s[t] = x
    return jnp.concatenate(s, axis=0)


def split3(x):
    a = x.astype(jnp.bfloat16)
    x = x - a.astype(jnp.float32)
    b = x.astype(jnp.bfloat16)
    return a, b, (x - b.astype(jnp.float32)).astype(jnp.bfloat16)


def lhs_terms(x):
    a, b, c = split3(x)
    return jnp.concatenate([a, a, b, a, c, b], axis=1)


def rhs_terms(x):
    a, b, c = split3(x)
    return jnp.concatenate([a, b, a, c, a, b], axis=0)


def invert_diagonal(d_ref):
    lane = iota((128, 128), 1)
    lane32 = iota((32, 128), 1)
    segment = lane32 // 32
    pad = jnp.zeros((64, 128), jnp.bfloat16)
    for q in range(4):
        lo, hi = 32 * q, 32 * q + 32
        packed = jnp.zeros((32, 128), jnp.float32)
        for c in range(4):
            rows = d_ref[c, lo:hi, :]
            moved = pltpu.roll(rows, (32 * (c - q)) % 128, 1) if c != q else rows
            packed = jnp.where(segment == c, moved, packed)
        packed = packed_inverse(packed)
        turned = [packed] + [pltpu.roll(packed, 32 * t, 1) for t in range(1, 4)]
        in_cols = (lane >= lo) & (lane < hi)
        in_lanes = segment == q
        for c in range(4):
            inverse = turned[(0 - c) % 4]
            for t in range(1, 4):
                inverse = jnp.where(segment == t, turned[(t - c) % 4], inverse)
            a, b, e = split3(inverse)
            none = jnp.zeros_like(a)
            lhs = jnp.concatenate(
                [
                    jnp.where(segment == 2, b, a),
                    jnp.where(segment == 0, e, jnp.where(segment == 1, b, none)),
                ],
                axis=1,
            )
            rows = d_ref[c, lo:hi, :]
            rhs = jnp.concatenate([rhs_terms(rows), pad], axis=0)
            scaled = jnp.dot(lhs, rhs, preferred_element_type=jnp.float32)
            scaled = jnp.where(in_lanes, inverse, scaled)
            a, b, e = split3(jnp.where(in_lanes, 0.0, jnp.where(lane32 < lo, rows, -rows)))
            lhs = jnp.concatenate([a, a, b, a, e, b, pad], axis=0)
            rhs = jnp.concatenate([rhs_terms(scaled), pad], axis=0)
            change = lax.dot_general(
                lhs, rhs, (((0,), (0,)), ((), ())), preferred_element_type=jnp.float32
            )
            d_ref[c] = jnp.where(in_cols, 0.0, d_ref[c]) + change
            d_ref[c, lo:hi, :] = scaled


def solve_kernel(g_ref, interp_ref, w_ref, d_ref):
    clusters, width = g_ref.shape[0], g_ref.shape[2]
    w_ref[...] = g_ref[...]
    for s in range(K // 128):
        lo, hi = 128 * s, 128 * s + 128
        for c in range(clusters):
            d_ref[c] = w_ref[c, lo:hi, lo:hi]
        invert_diagonal(d_ref)

        def one(c, carry):
            scaled = jnp.dot(
                lhs_terms(d_ref[c]), rhs_terms(w_ref[c, lo:hi, hi:]), preferred_element_type=jnp.float32
            )
            terms = rhs_terms(scaled)
            out = interp_ref if hi == K else w_ref
            out[c, lo:hi, 0 if hi == K else hi :] = scaled
            for t in range(K // 128):
                if t != s:
                    rows = slice(128 * t, 128 * t + 128)
                    rest = w_ref[c, rows, hi:] - jnp.dot(
                        lhs_terms(w_ref[c, rows, lo:hi]), terms, preferred_element_type=jnp.float32
                    )
                    out[c, rows, 0 if hi == K else hi :] = rest
            return carry

        lax.fori_loop(0, clusters, one, 0)


def solve(gram):
    clusters, kept, width = gram.shape
    vmem = pl.BlockSpec(memory_space=pltpu.VMEM)
    return pl.pallas_call(
        solve_kernel,
        out_shape=jax.ShapeDtypeStruct((clusters, kept, width - kept), jnp.float32),
        in_specs=[vmem],
        out_specs=vmem,
        scratch_shapes=[
            pltpu.VMEM((clusters, kept, width), jnp.float32),
            pltpu.VMEM((clusters, 128, 128), jnp.float32),
        ],
        compiler_params=pltpu.CompilerParams(vmem_limit_bytes=56 * 1024 * 1024),
        name="solve",
    )(gram)


PACKED = 648


def mirrored(low):
    at = iota(low.shape, 0) >= iota(low.shape, 1)
    return jnp.where(at, low, low.T)


def schur_kernel(n_ref, interp_ref, o_ref, own_ref, send_sem, recv_sems, *sides):
    clusters = own_ref.shape[0]
    places = []
    for axis in ("gx", "yz"):
        here, size = lax.axis_index(axis), lax.axis_size(axis)
        places += [(axis, here - 1, here > 0), (axis, here + 1, here < size - 1)]
    barrier = pltpu.get_barrier_semaphore()
    for axis, to, there in places:

        @pl.when(there)
        def _():
            pl.semaphore_signal(
                barrier, inc=1, device_id={axis: to}, device_id_type=pl.DeviceIdType.MESH
            )

    count = sum(there.astype(jnp.int32) for _, _, there in places)
    row, col = iota((128, 128), 0), iota((128, 128), 1)

    def make(c):
        a, b, _ = split3(interp_ref[c])
        lhs = jnp.concatenate([a, a, b], axis=1)
        rhs = jnp.concatenate([a, b, a], axis=1)
        across = (((1,), (1,)), ((), ()))
        left = lax.dot_general(lhs, rhs[:256], across, preferred_element_type=jnp.float32)
        last = lax.dot_general(lhs[256:], rhs[256:], across, preferred_element_type=jnp.float32)
        own_ref[c, :256] = left[128:, :128]
        own_ref[c, 256:384] = left[256:, 128:]
        middle = left[128:256, 128:]
        own_ref[c, 384:512] = jnp.where(row >= col, left[:128, :128], middle)
        own_ref[c, 512:640] = last
        diagonal = jnp.sum(jnp.where(row == col, middle, 0.0), axis=0, keepdims=True)
        own_ref[c, 640:648] = jnp.broadcast_to(diagonal, (8, 128))

    def copy(c, n):
        axis, to, _ = places[n]
        return pltpu.make_async_remote_copy(
            src_ref=own_ref.at[c],
            dst_ref=sides[n ^ 1].at[c],
            send_sem=send_sem.at[n],
            recv_sem=recv_sems.at[n ^ 1],
            device_id={axis: to},
            device_id_type=pl.DeviceIdType.MESH,
        )

    make(0)
    pl.semaphore_wait(barrier, count)
    for c in range(clusters):
        for n in (2, 3, 0, 1):
            pl.when(places[n][2])(lambda: copy(c, n).start())
        if c + 1 < clusters:
            make(c + 1)

    def settle(sem):
        pltpu.make_async_copy(own_ref, own_ref, sem).wait()

    for n in range(4):
        pl.when(places[n][2])(lambda: settle(recv_sems.at[n]))

    def add(c, carry):
        total = own_ref[c]
        for n in range(4):
            total = total + jnp.where(places[n][2], sides[n][n_ref[c, n]], 0.0)
        for at, i, j in ((0, 1, 0), (128, 2, 0), (256, 2, 1)):
            x = total[at : at + 128]
            o_ref[c, 128 * i : 128 * i + 128, 128 * j : 128 * j + 128] = x
            o_ref[c, 128 * j : 128 * j + 128, 128 * i : 128 * i + 128] = x.T
        both, last = total[384:512], total[512:640]
        o_ref[c, :128, :128] = mirrored(both)
        o_ref[c, 128:256, 128:256] = jnp.where(row == col, total[640:641], mirrored(both.T))
        o_ref[c, 256:, 256:] = mirrored(last)
        return carry

    lax.fori_loop(0, clusters, add, 0)
    for n in range(4):
        pl.when(places[n][2])(lambda: settle(send_sem.at[n]))


def schur_of(interp, neighbours):
    clusters = interp.shape[0]
    vmem = pl.BlockSpec(memory_space=pltpu.VMEM)
    packed = pltpu.VMEM((clusters, PACKED, 128), jnp.float32)
    return pl.pallas_call(
        schur_kernel,
        out_shape=jax.ShapeDtypeStruct((clusters, K, K), jnp.float32),
        in_specs=[pl.BlockSpec(memory_space=pltpu.SMEM), vmem],
        out_specs=vmem,
        scratch_shapes=[packed, pltpu.SemaphoreType.DMA((4,)), pltpu.SemaphoreType.DMA((4,))] + [packed] * 4,
        compiler_params=pltpu.CompilerParams(
            collective_id=1, has_side_effects=True, vmem_limit_bytes=40 * 1024 * 1024
        ),
        name="update_schur",
    )(neighbours, interp)


def body(fine_blocks, fine_to_coarse, widths, pivots, neighbours):
    gx_count, yz_count = lax.axis_size("gx"), lax.axis_size("yz")
    gx_pos, yz_pos = lax.axis_index("gx"), lax.axis_index("yz")
    blocks_dev = fine_blocks.shape[0]
    clusters = blocks_dev // 2
    grouped = lax.dynamic_index_in_dim(
        fine_to_coarse.reshape(gx_count, yz_count, blocks_dev), gx_pos, 0, keepdims=False
    )
    owner, local = grouped // clusters - gx_pos * yz_count, grouped % clusters
    target = lax.dynamic_index_in_dim(owner, yz_pos, 0, keepdims=False)
    mine = (owner == yz_pos)[None] & (local[None] == jnp.arange(clusters, dtype=jnp.int32)[:, None, None])
    peer = jnp.arange(yz_count, dtype=jnp.int32)[None, :, None]
    first = jnp.min(jnp.where(mine, peer, yz_count - 1), axis=(1, 2))
    second = jnp.max(jnp.where(mine, peer, 0), axis=(1, 2))
    goes = target[None, :] == jnp.arange(yz_count, dtype=jnp.int32)[:, None]
    numbers = jnp.stack([jnp.arange(blocks_dev, dtype=jnp.int32), widths])
    slots = jnp.sum(jnp.where(goes[None], numbers[:, None, :], 0), axis=2)
    interp = solve(exchange_gram(fine_blocks, slots, jnp.stack([first, second]), pivots))
    return interp, schur_of(interp, neighbours)


def solution(mesh):
    split = ("gx", "yz")
    return jax.shard_map(
        body,
        mesh=mesh,
        in_specs=(P(split, None, None), P(), P(split), P(split, None), P(split, None)),
        out_specs=(P(split, None, None), P(split, None, None)),
        check_vma=False,
    )
```

```python
import functools

import jax
import jax.numpy as jnp
from jax import lax
from jax.experimental import pallas as pl
from jax.experimental.pallas import tpu as pltpu
from jax.sharding import PartitionSpec as P

K = 384
HIGH = lax.Precision.HIGHEST


def iota(shape, dim):
    return lax.broadcasted_iota(jnp.int32, shape, dim)


SHARES = (1, 2, 2, 2, 2, 2, 1)
STARTS = tuple(sum(SHARES[:n]) for n in range(len(SHARES)))
GROUPS, STAGES = len(SHARES), 3


def exchange_gram_kernel(
    sel_ref, slot_ref, x_ref, piv_ref, g_ref, o_ref, hot_ref, send_sems, recv_sems, in_sems, out_sems, *bufs
):
    lands, slots, blocks = bufs[:GROUPS], bufs[GROUPS : GROUPS + STAGES], bufs[GROUPS + STAGES :]
    me = lax.axis_index("yz")
    plane = lax.axis_size("yz")
    side = 4
    clusters, kept, width = o_ref.shape
    peers, unit, half = lands[0].shape
    step = unit // 2

    def peer(d):
        return lax.rem(me // side + d // side, plane // side) * side + lax.rem(me + d, side)

    def done(c):
        return pltpu.make_async_copy(o_ref.at[c], g_ref.at[c], out_sems.at[c])

    def fetch(group):
        height = SHARES[group] * unit
        return pltpu.make_async_copy(
            x_ref.at[:, pl.ds(STARTS[group] * unit, height)],
            blocks[group % 2].at[:, pl.ds(0, height)],
            in_sems.at[group % 2],
        )

    fetch(0).start()
    fetch(1).start()
    barrier = pltpu.get_barrier_semaphore()

    def greet(d, carry):
        pl.semaphore_signal(
            barrier, inc=1, device_id={"yz": peer(d)}, device_id_type=pl.DeviceIdType.MESH
        )
        return carry

    lax.fori_loop(1, peers, greet, 0)

    def sent(group):
        rest = slots[group % STAGES].at[pl.ds(0, peers - 1), pl.ds(0, SHARES[group] * unit)]
        pltpu.make_async_copy(rest, rest, send_sems.at[group % STAGES]).wait()

    def fill(group):
        fetch(group).wait()
        if group >= STAGES:
            sent(group - STAGES)
        height = SHARES[group] * unit
        column = iota((height, half), 1)

        def masked(t):
            x = blocks[group % 2][slot_ref[0, t], :height]
            return jnp.where(column < slot_ref[1, t], x, jnp.zeros_like(x))

        def one(d, carry):
            slots[group % STAGES][peer(d), :height] = masked(peer(d))
            return carry

        lax.fori_loop(1, peers, one, 0)
        lands[group][me] = masked(me)
        if group + 2 < GROUPS:
            fetch(group + 2).start()

    def launch(group):
        def one(n, carry):
            piece, to = n // (peers - 1), peer(1 + lax.rem(n, peers - 1))
            rows = pl.ds(pl.multiple_of(piece * step, step), step)
            pltpu.make_async_remote_copy(
                src_ref=slots[group % STAGES].at[to, rows],
                dst_ref=lands[group].at[me, rows],
                send_sem=send_sems.at[group % STAGES],
                recv_sem=recv_sems.at[group],
                device_id={"yz": to},
                device_id_type=pl.DeviceIdType.MESH,
            ).start()
            return carry

        lax.fori_loop(0, SHARES[group] * unit // step * (peers - 1), one, 0)

    fill(0)
    pl.semaphore_wait(barrier, peers - 1)
    launch(0)
    fill(1)
    launch(1)

    def make_hot(c, carry):
        hot_ref[c] = jnp.where(iota((width, width), 0) == piv_ref[pl.ds(c, 1), :], 1.0, 0.0).astype(hot_ref.dtype)
        return carry

    lax.fori_loop(0, clusters, make_hot, 0)
    fill(2)

    for group in range(GROUPS):
        land = lands[group]
        rest = land.at[pl.ds(0, peers - 1)]
        pltpu.make_async_copy(rest, rest, recv_sems.at[group]).wait()
        if group + 2 < GROUPS:
            launch(group + 2)

        def one_cluster(c, carry):
            a, b = land[sel_ref[0, c]], land[sel_ref[1, c]]
            pivoted = jnp.dot(a, hot_ref[c, :half, :], preferred_element_type=jnp.float32)
            pivoted += jnp.dot(b, hot_ref[c, half:, :], preferred_element_type=jnp.float32)
            pivoted = pivoted.astype(jnp.bfloat16)
            part = lax.dot_general(
                pivoted[:, :kept], pivoted, (((0,), (0,)), ((), ())), preferred_element_type=jnp.float32
            )
            o_ref[c] = part if group == 0 else o_ref[c] + part
            if group == GROUPS - 1:
                done(c).start()
            return carry

        lax.fori_loop(0, clusters, one_cluster, 0)
        if group + STAGES < GROUPS:
            fill(group + STAGES)

    for group in range(GROUPS - STAGES, GROUPS):
        sent(group)
    for c in range(clusters):
        done(c).wait()


def exchange_gram(fine_blocks, slots, chosen, pivots):
    count, rows, half = fine_blocks.shape
    peers = slots.shape[1]
    clusters, width = pivots.shape
    unit = rows // sum(SHARES)
    vmem, smem = pl.BlockSpec(memory_space=pltpu.VMEM), pl.BlockSpec(memory_space=pltpu.SMEM)
    return pl.pallas_call(
        exchange_gram_kernel,
        out_shape=jax.ShapeDtypeStruct((clusters, K, width), jnp.float32),
        in_specs=[smem, smem, pl.BlockSpec(memory_space=pltpu.HBM), vmem],
        out_specs=pl.BlockSpec(memory_space=pltpu.HBM),
        scratch_shapes=[
            pltpu.VMEM((clusters, K, width), jnp.float32),
            pltpu.VMEM((clusters, width, width), jnp.bfloat16),
            pltpu.SemaphoreType.DMA((STAGES,)),
            pltpu.SemaphoreType.DMA((GROUPS,)),
            pltpu.SemaphoreType.DMA((2,)),
            pltpu.SemaphoreType.DMA((clusters,)),
        ]
        + [pltpu.VMEM((peers, share * unit, half), jnp.bfloat16) for share in SHARES]
        + [pltpu.VMEM((peers, max(SHARES) * unit, half), jnp.bfloat16) for _ in range(STAGES)]
        + [pltpu.VMEM((count, max(SHARES) * unit, half), jnp.bfloat16) for _ in range(2)],
        compiler_params=pltpu.CompilerParams(
            collective_id=0, has_side_effects=True, vmem_limit_bytes=63 * 1024 * 1024
        ),
        name="exchange_gram",
    )(chosen, slots, fine_blocks, pivots)


def packed_inverse(s):
    lane, row = iota((8, 128), 1), iota((8, 128), 0)
    inner = lane % 32
    base = lane - inner
    s = [s[8 * t : 8 * t + 8] for t in range(4)]

    def spread(x, k):
        return jnp.broadcast_to(x[k % 8 : k % 8 + 1], (8, 128))

    for k in range(0, 32, 4):
        at = k // 8
        cols = [
            [jnp.take_along_axis(x, base + (k + j), axis=1, mode="promise_in_bounds") for x in s]
            for j in range(4)
        ]
        here = (inner >= k) & (inner < k + 4)
        d = [[spread(cols[j][at], k + i) for j in range(4)] for i in range(4)]
        w = [jnp.where(here, jnp.where(inner == k + i, 1.0, 0.0), spread(s[at], k + i)) for i in range(4)]
        for p in range(4):
            scale = 1.0 / d[p][p]
            w[p] = w[p] * scale
            for j in range(p + 1, 4):
                d[p][j] = d[p][j] * scale
            for i in range(4):
                if i != p:
                    w[i] = w[i] - d[i][p] * w[p]
                    for j in range(p + 1, 4):
                        d[i][j] = d[i][j] - d[i][p] * d[p][j]
        for t in range(4):
            x = jnp.where(here, 0.0, s[t])
            x = x - (cols[0][t] * w[0] + cols[1][t] * w[1]) - (cols[2][t] * w[2] + cols[3][t] * w[3])
            if t == at:
                for i in range(4):
                    x = jnp.where(row == (k + i) % 8, w[i], x)
            s[t] = x
    return jnp.concatenate(s, axis=0)


def split3(x):
    a = x.astype(jnp.bfloat16)
    x = x - a.astype(jnp.float32)
    b = x.astype(jnp.bfloat16)
    return a, b, (x - b.astype(jnp.float32)).astype(jnp.bfloat16)


def lhs_terms(x):
    a, b, c = split3(x)
    return jnp.concatenate([a, a, b, a, c, b], axis=1)


def rhs_terms(x):
    a, b, c = split3(x)
    return jnp.concatenate([a, b, a, c, a, b], axis=0)


def invert_diagonal(d_ref):
    lane = iota((128, 128), 1)
    lane32 = iota((32, 128), 1)
    segment = lane32 // 32
    pad = jnp.zeros((64, 128), jnp.bfloat16)
    for q in range(4):
        lo, hi = 32 * q, 32 * q + 32
        packed = jnp.zeros((32, 128), jnp.float32)
        for c in range(4):
            rows = d_ref[c, lo:hi, :]
            moved = pltpu.roll(rows, (32 * (c - q)) % 128, 1) if c != q else rows
            packed = jnp.where(segment == c, moved, packed)
        packed = packed_inverse(packed)
        turned = [packed] + [pltpu.roll(packed, 32 * t, 1) for t in range(1, 4)]
        in_cols = (lane >= lo) & (lane < hi)
        in_lanes = segment == q
        for c in range(4):
            inverse = turned[(0 - c) % 4]
            for t in range(1, 4):
                inverse = jnp.where(segment == t, turned[(t - c) % 4], inverse)
            a, b, e = split3(inverse)
            none = jnp.zeros_like(a)
            lhs = jnp.concatenate(
                [
                    jnp.where(segment == 2, b, a),
                    jnp.where(segment == 0, e, jnp.where(segment == 1, b, none)),
                ],
                axis=1,
            )
            rows = d_ref[c, lo:hi, :]
            rhs = jnp.concatenate([rhs_terms(rows), pad], axis=0)
            scaled = jnp.dot(lhs, rhs, preferred_element_type=jnp.float32)
            scaled = jnp.where(in_lanes, inverse, scaled)
            a, b, e = split3(jnp.where(in_lanes, 0.0, jnp.where(lane32 < lo, rows, -rows)))
            lhs = jnp.concatenate([a, a, b, a, e, b, pad], axis=0)
            rhs = jnp.concatenate([rhs_terms(scaled), pad], axis=0)
            change = lax.dot_general(
                lhs, rhs, (((0,), (0,)), ((), ())), preferred_element_type=jnp.float32
            )
            d_ref[c] = jnp.where(in_cols, 0.0, d_ref[c]) + change
            d_ref[c, lo:hi, :] = scaled


def solve_kernel(g_ref, interp_ref, w_ref, d_ref, sems):
    clusters = g_ref.shape[0]
    first = pltpu.make_async_copy(g_ref.at[:, pl.ds(0, 128), pl.ds(0, 128)], d_ref, sems.at[0])
    rest = pltpu.make_async_copy(g_ref, w_ref, sems.at[1])
    first.start()
    rest.start()
    first.wait()
    for s in range(K // 128):
        lo, hi = 128 * s, 128 * s + 128
        if s > 0:
            for c in range(clusters):
                d_ref[c] = w_ref[c, lo:hi, lo:hi]
        invert_diagonal(d_ref)
        if s == 0:
            rest.wait()

        def one(c, carry):
            scaled = jnp.dot(
                lhs_terms(d_ref[c]), rhs_terms(w_ref[c, lo:hi, hi:]), preferred_element_type=jnp.float32
            )
            terms = rhs_terms(scaled)
            out = interp_ref if hi == K else w_ref
            out[c, lo:hi, 0 if hi == K else hi :] = scaled
            for t in range(K // 128):
                if t != s:
                    rows = slice(128 * t, 128 * t + 128)
                    rest = w_ref[c, rows, hi:] - jnp.dot(
                        lhs_terms(w_ref[c, rows, lo:hi]), terms, preferred_element_type=jnp.float32
                    )
                    out[c, rows, 0 if hi == K else hi :] = rest
            return carry

        lax.fori_loop(0, clusters, one, 0)


def solve(gram):
    clusters, kept, width = gram.shape
    vmem = pl.BlockSpec(memory_space=pltpu.VMEM)
    return pl.pallas_call(
        solve_kernel,
        out_shape=jax.ShapeDtypeStruct((clusters, kept, width - kept), jnp.float32),
        in_specs=[pl.BlockSpec(memory_space=pltpu.HBM)],
        out_specs=vmem,
        scratch_shapes=[
            pltpu.VMEM((clusters, kept, width), jnp.float32),
            pltpu.VMEM((clusters, 128, 128), jnp.float32),
            pltpu.SemaphoreType.DMA((2,)),
        ],
        compiler_params=pltpu.CompilerParams(vmem_limit_bytes=56 * 1024 * 1024),
        name="solve",
    )(gram)


PACKED = 648


def mirrored(low):
    at = iota(low.shape, 0) >= iota(low.shape, 1)
    return jnp.where(at, low, low.T)


def schur_kernel(n_ref, interp_ref, o_ref, x_ref, own_ref, in_sems, send_sem, recv_sems, *sides):
    clusters = own_ref.shape[0]

    def fetch(c):
        return pltpu.make_async_copy(interp_ref.at[c], x_ref.at[c], in_sems.at[c])

    for c in range(clusters):
        fetch(c).start()
    places = []
    for axis in ("gx", "yz"):
        here, size = lax.axis_index(axis), lax.axis_size(axis)
        places += [(axis, here - 1, here > 0), (axis, here + 1, here < size - 1)]
    barrier = pltpu.get_barrier_semaphore()
    for axis, to, there in places:

        @pl.when(there)
        def _():
            pl.semaphore_signal(
                barrier, inc=1, device_id={axis: to}, device_id_type=pl.DeviceIdType.MESH
            )

    count = sum(there.astype(jnp.int32) for _, _, there in places)
    row, col = iota((128, 128), 0), iota((128, 128), 1)

    def make(c):
        fetch(c).wait()
        a, b, _ = split3(x_ref[c])
        lhs = jnp.concatenate([a, a, b], axis=1)
        rhs = jnp.concatenate([a, b, a], axis=1)
        across = (((1,), (1,)), ((), ()))
        left = lax.dot_general(lhs, rhs[:256], across, preferred_element_type=jnp.float32)
        last = lax.dot_general(lhs[256:], rhs[256:], across, preferred_element_type=jnp.float32)
        own_ref[c, :256] = left[128:, :128]
        own_ref[c, 256:384] = left[256:, 128:]
        middle = left[128:256, 128:]
        own_ref[c, 384:512] = jnp.where(row >= col, left[:128, :128], middle)
        own_ref[c, 512:640] = last
        diagonal = jnp.sum(jnp.where(row == col, middle, 0.0), axis=0, keepdims=True)
        own_ref[c, 640:648] = jnp.broadcast_to(diagonal, (8, 128))

    def copy(c, n):
        axis, to, _ = places[n]
        return pltpu.make_async_remote_copy(
            src_ref=own_ref.at[c],
            dst_ref=sides[n ^ 1].at[c],
            send_sem=send_sem.at[n],
            recv_sem=recv_sems.at[n ^ 1],
            device_id={axis: to},
            device_id_type=pl.DeviceIdType.MESH,
        )

    make(0)
    pl.semaphore_wait(barrier, count)
    for c in range(clusters):
        for n in (2, 3, 0, 1):
            pl.when(places[n][2])(lambda: copy(c, n).start())
        if c + 1 < clusters:
            make(c + 1)

    def settle(sem):
        pltpu.make_async_copy(own_ref, own_ref, sem).wait()

    for n in range(4):
        pl.when(places[n][2])(lambda: settle(recv_sems.at[n]))

    def add(c, carry):
        total = own_ref[c]
        for n in range(4):
            total = total + jnp.where(places[n][2], sides[n][n_ref[c, n]], 0.0)
        for at, i, j in ((0, 1, 0), (128, 2, 0), (256, 2, 1)):
            x = total[at : at + 128]
            o_ref[c, 128 * i : 128 * i + 128, 128 * j : 128 * j + 128] = x
            o_ref[c, 128 * j : 128 * j + 128, 128 * i : 128 * i + 128] = x.T
        both, last = total[384:512], total[512:640]
        o_ref[c, :128, :128] = mirrored(both)
        o_ref[c, 128:256, 128:256] = jnp.where(row == col, total[640:641], mirrored(both.T))
        o_ref[c, 256:, 256:] = mirrored(last)
        return carry

    lax.fori_loop(0, clusters, add, 0)
    for n in range(4):
        pl.when(places[n][2])(lambda: settle(send_sem.at[n]))


def schur_of(interp, neighbours):
    clusters = interp.shape[0]
    vmem = pl.BlockSpec(memory_space=pltpu.VMEM)
    packed = pltpu.VMEM((clusters, PACKED, 128), jnp.float32)
    return pl.pallas_call(
        schur_kernel,
        out_shape=jax.ShapeDtypeStruct((clusters, K, K), jnp.float32),
        in_specs=[pl.BlockSpec(memory_space=pltpu.SMEM), pl.BlockSpec(memory_space=pltpu.HBM)],
        out_specs=vmem,
        scratch_shapes=[
            pltpu.VMEM(interp.shape, jnp.float32),
            packed,
            pltpu.SemaphoreType.DMA((clusters,)),
            pltpu.SemaphoreType.DMA((4,)),
            pltpu.SemaphoreType.DMA((4,)),
        ]
        + [packed] * 4,
        compiler_params=pltpu.CompilerParams(
            collective_id=1, has_side_effects=True, vmem_limit_bytes=62 * 1024 * 1024
        ),
        name="update_schur",
    )(neighbours, interp)


def body(fine_blocks, fine_to_coarse, widths, pivots, neighbours):
    gx_count, yz_count = lax.axis_size("gx"), lax.axis_size("yz")
    gx_pos, yz_pos = lax.axis_index("gx"), lax.axis_index("yz")
    blocks_dev = fine_blocks.shape[0]
    clusters = blocks_dev // 2
    grouped = lax.dynamic_index_in_dim(
        fine_to_coarse.reshape(gx_count, yz_count, blocks_dev), gx_pos, 0, keepdims=False
    )
    owner, local = grouped // clusters - gx_pos * yz_count, grouped % clusters
    target = lax.dynamic_index_in_dim(owner, yz_pos, 0, keepdims=False)
    mine = (owner == yz_pos)[None] & (local[None] == jnp.arange(clusters, dtype=jnp.int32)[:, None, None])
    peer = jnp.arange(yz_count, dtype=jnp.int32)[None, :, None]
    first = jnp.min(jnp.where(mine, peer, yz_count - 1), axis=(1, 2))
    second = jnp.max(jnp.where(mine, peer, 0), axis=(1, 2))
    goes = target[None, :] == jnp.arange(yz_count, dtype=jnp.int32)[:, None]
    numbers = jnp.stack([jnp.arange(blocks_dev, dtype=jnp.int32), widths])
    slots = jnp.sum(jnp.where(goes[None], numbers[:, None, :], 0), axis=2)
    interp = solve(exchange_gram(fine_blocks, slots, jnp.stack([first, second]), pivots))
    return interp, schur_of(interp, neighbours)


def solution(mesh):
    split = ("gx", "yz")
    return jax.shard_map(
        body,
        mesh=mesh,
        in_specs=(P(split, None, None), P(), P(split), P(split, None), P(split, None)),
        out_specs=(P(split, None, None), P(split, None, None)),
        check_vma=False,
    )
```

```python
import functools

import jax
import jax.numpy as jnp
from jax import lax
from jax.experimental import pallas as pl
from jax.experimental.pallas import tpu as pltpu
from jax.sharding import PartitionSpec as P

K = 384
HIGH = lax.Precision.HIGHEST


def iota(shape, dim):
    return lax.broadcasted_iota(jnp.int32, shape, dim)


SHARES = (1, 2, 2, 2, 2, 2, 1)
STARTS = tuple(sum(SHARES[:n]) for n in range(len(SHARES)))
GROUPS, STAGES = len(SHARES), 3


def exchange_gram_kernel(
    sel_ref, slot_ref, x_ref, piv_ref, g_ref, o_ref, hot_ref, send_sems, recv_sems, in_sems, out_sems, *bufs
):
    lands, slots, blocks = bufs[:GROUPS], bufs[GROUPS : GROUPS + STAGES], bufs[GROUPS + STAGES :]
    me = lax.axis_index("yz")
    plane = lax.axis_size("yz")
    side = 4
    clusters, kept, width = o_ref.shape
    peers, unit, half = lands[0].shape
    step = unit // 2

    def peer(d):
        return lax.rem(me // side + d // side, plane // side) * side + lax.rem(me + d, side)

    def done(c):
        return pltpu.make_async_copy(o_ref.at[c], g_ref.at[c], out_sems.at[c])

    def fetch(group):
        height = SHARES[group] * unit
        return pltpu.make_async_copy(
            x_ref.at[:, pl.ds(STARTS[group] * unit, height)],
            blocks[group % 2].at[:, pl.ds(0, height)],
            in_sems.at[group % 2],
        )

    fetch(0).start()
    fetch(1).start()
    barrier = pltpu.get_barrier_semaphore()

    def greet(d, carry):
        pl.semaphore_signal(
            barrier, inc=1, device_id={"yz": peer(d)}, device_id_type=pl.DeviceIdType.MESH
        )
        return carry

    lax.fori_loop(1, peers, greet, 0)

    def sent(group):
        rest = slots[group % STAGES].at[pl.ds(0, peers - 1), pl.ds(0, SHARES[group] * unit)]
        pltpu.make_async_copy(rest, rest, send_sems.at[group % STAGES]).wait()

    def fill(group):
        fetch(group).wait()
        if group >= STAGES:
            sent(group - STAGES)
        height = SHARES[group] * unit
        column = iota((height, half), 1)

        def masked(t):
            x = blocks[group % 2][slot_ref[0, t], :height]
            return jnp.where(column < slot_ref[1, t], x, jnp.zeros_like(x))

        def one(d, carry):
            slots[group % STAGES][peer(d), :height] = masked(peer(d))
            return carry

        lax.fori_loop(1, peers, one, 0)
        lands[group][me] = masked(me)
        if group + 2 < GROUPS:
            fetch(group + 2).start()

    def launch(group):
        def one(n, carry):
            piece, to = n // (peers - 1), peer(1 + lax.rem(n, peers - 1))
            rows = pl.ds(pl.multiple_of(piece * step, step), step)
            pltpu.make_async_remote_copy(
                src_ref=slots[group % STAGES].at[to, rows],
                dst_ref=lands[group].at[me, rows],
                send_sem=send_sems.at[group % STAGES],
                recv_sem=recv_sems.at[group],
                device_id={"yz": to},
                device_id_type=pl.DeviceIdType.MESH,
            ).start()
            return carry

        lax.fori_loop(0, SHARES[group] * unit // step * (peers - 1), one, 0)

    fill(0)
    pl.semaphore_wait(barrier, peers - 1)
    launch(0)
    fill(1)
    launch(1)

    def make_hot(c, carry):
        hot_ref[c] = jnp.where(iota((width, width), 0) == piv_ref[pl.ds(c, 1), :], 1.0, 0.0).astype(hot_ref.dtype)
        return carry

    lax.fori_loop(0, clusters, make_hot, 0)
    fill(2)

    for group in range(GROUPS):
        land = lands[group]
        rest = land.at[pl.ds(0, peers - 1)]
        pltpu.make_async_copy(rest, rest, recv_sems.at[group]).wait()
        if group + 2 < GROUPS:
            launch(group + 2)

        def one_cluster(c, carry):
            a, b = land[sel_ref[0, c]], land[sel_ref[1, c]]
            pivoted = jnp.dot(a, hot_ref[c, :half, :], preferred_element_type=jnp.float32)
            pivoted += jnp.dot(b, hot_ref[c, half:, :], preferred_element_type=jnp.float32)
            pivoted = pivoted.astype(jnp.bfloat16)
            part = lax.dot_general(
                pivoted[:, :kept], pivoted, (((0,), (0,)), ((), ())), preferred_element_type=jnp.float32
            )
            o_ref[c] = part if group == 0 else o_ref[c] + part
            if group == GROUPS - 1:
                done(c).start()
            return carry

        lax.fori_loop(0, clusters, one_cluster, 0)
        if group + STAGES < GROUPS:
            fill(group + STAGES)

    for group in range(GROUPS - STAGES, GROUPS):
        sent(group)
    for c in range(clusters):
        done(c).wait()


def exchange_gram(fine_blocks, slots, chosen, pivots):
    count, rows, half = fine_blocks.shape
    peers = slots.shape[1]
    clusters, width = pivots.shape
    unit = rows // sum(SHARES)
    vmem, smem = pl.BlockSpec(memory_space=pltpu.VMEM), pl.BlockSpec(memory_space=pltpu.SMEM)
    return pl.pallas_call(
        exchange_gram_kernel,
        out_shape=jax.ShapeDtypeStruct((clusters, K, width), jnp.float32),
        in_specs=[smem, smem, pl.BlockSpec(memory_space=pltpu.HBM), vmem],
        out_specs=pl.BlockSpec(memory_space=pltpu.HBM),
        scratch_shapes=[
            pltpu.VMEM((clusters, K, width), jnp.float32),
            pltpu.VMEM((clusters, width, width), jnp.bfloat16),
            pltpu.SemaphoreType.DMA((STAGES,)),
            pltpu.SemaphoreType.DMA((GROUPS,)),
            pltpu.SemaphoreType.DMA((2,)),
            pltpu.SemaphoreType.DMA((clusters,)),
        ]
        + [pltpu.VMEM((peers, share * unit, half), jnp.bfloat16) for share in SHARES]
        + [pltpu.VMEM((peers, max(SHARES) * unit, half), jnp.bfloat16) for _ in range(STAGES)]
        + [pltpu.VMEM((count, max(SHARES) * unit, half), jnp.bfloat16) for _ in range(2)],
        compiler_params=pltpu.CompilerParams(
            collective_id=0, has_side_effects=True, vmem_limit_bytes=63 * 1024 * 1024
        ),
        name="exchange_gram",
    )(chosen, slots, fine_blocks, pivots)


def packed_inverse(s):
    lane, row = iota((8, 128), 1), iota((8, 128), 0)
    inner = lane % 32
    base = lane - inner
    s = [s[8 * t : 8 * t + 8] for t in range(4)]

    def spread(x, k):
        return jnp.broadcast_to(x[k % 8 : k % 8 + 1], (8, 128))

    for k in range(0, 32, 4):
        at = k // 8
        cols = [
            [jnp.take_along_axis(x, base + (k + j), axis=1, mode="promise_in_bounds") for x in s]
            for j in range(4)
        ]
        here = (inner >= k) & (inner < k + 4)
        d = [[spread(cols[j][at], k + i) for j in range(4)] for i in range(4)]
        w = [jnp.where(here, jnp.where(inner == k + i, 1.0, 0.0), spread(s[at], k + i)) for i in range(4)]
        for p in range(4):
            scale = 1.0 / d[p][p]
            w[p] = w[p] * scale
            for j in range(p + 1, 4):
                d[p][j] = d[p][j] * scale
            for i in range(4):
                if i != p:
                    w[i] = w[i] - d[i][p] * w[p]
                    for j in range(p + 1, 4):
                        d[i][j] = d[i][j] - d[i][p] * d[p][j]
        for t in range(4):
            x = jnp.where(here, 0.0, s[t])
            x = x - (cols[0][t] * w[0] + cols[1][t] * w[1]) - (cols[2][t] * w[2] + cols[3][t] * w[3])
            if t == at:
                for i in range(4):
                    x = jnp.where(row == (k + i) % 8, w[i], x)
            s[t] = x
    return jnp.concatenate(s, axis=0)


def split3(x):
    a = x.astype(jnp.bfloat16)
    x = x - a.astype(jnp.float32)
    b = x.astype(jnp.bfloat16)
    return a, b, (x - b.astype(jnp.float32)).astype(jnp.bfloat16)


def lhs_terms(x):
    a, b, c = split3(x)
    return jnp.concatenate([a, a, b, a, c, b], axis=1)


def rhs_terms(x):
    a, b, c = split3(x)
    return jnp.concatenate([a, b, a, c, a, b], axis=0)


def invert_diagonal(d_ref):
    lane = iota((128, 128), 1)
    lane32 = iota((32, 128), 1)
    segment = lane32 // 32
    pad = jnp.zeros((64, 128), jnp.bfloat16)
    for q in range(4):
        lo, hi = 32 * q, 32 * q + 32
        packed = jnp.zeros((32, 128), jnp.float32)
        for c in range(4):
            rows = d_ref[c, lo:hi, :]
            moved = pltpu.roll(rows, (32 * (c - q)) % 128, 1) if c != q else rows
            packed = jnp.where(segment == c, moved, packed)
        packed = packed_inverse(packed)
        turned = [packed] + [pltpu.roll(packed, 32 * t, 1) for t in range(1, 4)]
        in_cols = (lane >= lo) & (lane < hi)
        in_lanes = segment == q
        for c in range(4):
            inverse = turned[(0 - c) % 4]
            for t in range(1, 4):
                inverse = jnp.where(segment == t, turned[(t - c) % 4], inverse)
            a, b, e = split3(inverse)
            none = jnp.zeros_like(a)
            lhs = jnp.concatenate(
                [
                    jnp.where(segment == 2, b, a),
                    jnp.where(segment == 0, e, jnp.where(segment == 1, b, none)),
                ],
                axis=1,
            )
            rows = d_ref[c, lo:hi, :]
            rhs = jnp.concatenate([rhs_terms(rows), pad], axis=0)
            scaled = jnp.dot(lhs, rhs, preferred_element_type=jnp.float32)
            scaled = jnp.where(in_lanes, inverse, scaled)
            a, b, e = split3(jnp.where(in_lanes, 0.0, jnp.where(lane32 < lo, rows, -rows)))
            lhs = jnp.concatenate([a, a, b, a, e, b, pad], axis=0)
            rhs = jnp.concatenate([rhs_terms(scaled), pad], axis=0)
            change = lax.dot_general(
                lhs, rhs, (((0,), (0,)), ((), ())), preferred_element_type=jnp.float32
            )
            d_ref[c] = jnp.where(in_cols, 0.0, d_ref[c]) + change
            d_ref[c, lo:hi, :] = scaled


def solve_kernel(g_ref, interp_ref, w_ref, d_ref, sems):
    clusters = g_ref.shape[0]
    first = pltpu.make_async_copy(g_ref.at[:, pl.ds(0, 128), pl.ds(0, 128)], d_ref, sems.at[0])
    rest = pltpu.make_async_copy(g_ref, w_ref, sems.at[1])
    first.start()
    rest.start()
    first.wait()
    for s in range(K // 128):
        lo, hi = 128 * s, 128 * s + 128
        if s > 0:
            for c in range(clusters):
                d_ref[c] = w_ref[c, lo:hi, lo:hi]
        invert_diagonal(d_ref)
        if s == 0:
            rest.wait()

        def one(c, carry):
            scaled = jnp.dot(
                lhs_terms(d_ref[c]), rhs_terms(w_ref[c, lo:hi, hi:]), preferred_element_type=jnp.float32
            )
            terms = rhs_terms(scaled)
            out = interp_ref if hi == K else w_ref
            out[c, lo:hi, 0 if hi == K else hi :] = scaled
            for t in range(K // 128):
                if t != s:
                    rows = slice(128 * t, 128 * t + 128)
                    rest = w_ref[c, rows, hi:] - jnp.dot(
                        lhs_terms(w_ref[c, rows, lo:hi]), terms, preferred_element_type=jnp.float32
                    )
                    out[c, rows, 0 if hi == K else hi :] = rest
            return carry

        lax.fori_loop(0, clusters, one, 0)


def solve(gram):
    clusters, kept, width = gram.shape
    vmem = pl.BlockSpec(memory_space=pltpu.VMEM)
    return pl.pallas_call(
        solve_kernel,
        out_shape=jax.ShapeDtypeStruct((clusters, kept, width - kept), jnp.float32),
        in_specs=[pl.BlockSpec(memory_space=pltpu.HBM)],
        out_specs=vmem,
        scratch_shapes=[
            pltpu.VMEM((clusters, kept, width), jnp.float32),
            pltpu.VMEM((clusters, 128, 128), jnp.float32),
            pltpu.SemaphoreType.DMA((2,)),
        ],
        compiler_params=pltpu.CompilerParams(vmem_limit_bytes=56 * 1024 * 1024),
        name="solve",
    )(gram)


PACKED = 648


def mirrored(low):
    at = iota(low.shape, 0) >= iota(low.shape, 1)
    return jnp.where(at, low, low.T)


def schur_kernel(n_ref, interp_ref, o_ref, x_ref, own_ref, in_sems, send_sem, recv_sems, *sides):
    clusters = own_ref.shape[0]

    def fetch(c):
        return pltpu.make_async_copy(interp_ref.at[c], x_ref.at[c], in_sems.at[c])

    for c in range(clusters):
        fetch(c).start()
    places = []
    for axis in ("gx", "yz"):
        here, size = lax.axis_index(axis), lax.axis_size(axis)
        places += [(axis, here - 1, here > 0), (axis, here + 1, here < size - 1)]
    barrier = pltpu.get_barrier_semaphore()
    for axis, to, there in places:

        @pl.when(there)
        def _():
            pl.semaphore_signal(
                barrier, inc=1, device_id={axis: to}, device_id_type=pl.DeviceIdType.MESH
            )

    count = sum(there.astype(jnp.int32) for _, _, there in places)
    row, col = iota((128, 128), 0), iota((128, 128), 1)

    def make(c):
        fetch(c).wait()
        a, b, _ = split3(x_ref[c])
        lhs = jnp.concatenate([a, a, b], axis=1)
        rhs = jnp.concatenate([a, b, a], axis=1)
        across = (((1,), (1,)), ((), ()))
        left = lax.dot_general(lhs, rhs[:256], across, preferred_element_type=jnp.float32)
        last = lax.dot_general(lhs[256:], rhs[256:], across, preferred_element_type=jnp.float32)
        own_ref[c, :256] = left[128:, :128]
        own_ref[c, 256:384] = left[256:, 128:]
        middle = left[128:256, 128:]
        own_ref[c, 384:512] = jnp.where(row >= col, left[:128, :128], middle)
        own_ref[c, 512:640] = last
        diagonal = jnp.sum(jnp.where(row == col, middle, 0.0), axis=0, keepdims=True)
        own_ref[c, 640:648] = jnp.broadcast_to(diagonal, (8, 128))

    def copy(c, n):
        axis, to, _ = places[n]
        return pltpu.make_async_remote_copy(
            src_ref=own_ref.at[c],
            dst_ref=sides[n ^ 1].at[c],
            send_sem=send_sem.at[n],
            recv_sem=recv_sems.at[n ^ 1],
            device_id={axis: to},
            device_id_type=pl.DeviceIdType.MESH,
        )

    make(0)
    pl.semaphore_wait(barrier, count)
    for c in range(clusters):
        for n in (2, 3, 0, 1):
            pl.when(places[n][2])(lambda: copy(c, n).start())
        if c + 1 < clusters:
            make(c + 1)

    def settle(sem):
        pltpu.make_async_copy(own_ref, own_ref, sem).wait()

    for n in range(4):
        pl.when(places[n][2])(lambda: settle(recv_sems.at[n]))

    def add(c, carry):
        total = own_ref[c]
        for n in range(4):
            total = total + jnp.where(places[n][2], sides[n][n_ref[c, n]], 0.0)
        for at, i, j in ((0, 1, 0), (128, 2, 0), (256, 2, 1)):
            x = total[at : at + 128]
            o_ref[c, 128 * i : 128 * i + 128, 128 * j : 128 * j + 128] = x
            o_ref[c, 128 * j : 128 * j + 128, 128 * i : 128 * i + 128] = x.T
        both, last = total[384:512], total[512:640]
        o_ref[c, :128, :128] = mirrored(both)
        o_ref[c, 128:256, 128:256] = jnp.where(row == col, total[640:641], mirrored(both.T))
        o_ref[c, 256:, 256:] = mirrored(last)
        return carry

    lax.fori_loop(0, clusters, add, 0)
    for n in range(4):
        pl.when(places[n][2])(lambda: settle(send_sem.at[n]))


def schur_of(interp, neighbours):
    clusters = interp.shape[0]
    vmem = pl.BlockSpec(memory_space=pltpu.VMEM)
    packed = pltpu.VMEM((clusters, PACKED, 128), jnp.float32)
    return pl.pallas_call(
        schur_kernel,
        out_shape=jax.ShapeDtypeStruct((clusters, K, K), jnp.float32),
        in_specs=[pl.BlockSpec(memory_space=pltpu.SMEM), pl.BlockSpec(memory_space=pltpu.HBM)],
        out_specs=vmem,
        scratch_shapes=[
            pltpu.VMEM(interp.shape, jnp.float32),
            packed,
            pltpu.SemaphoreType.DMA((clusters,)),
            pltpu.SemaphoreType.DMA((4,)),
            pltpu.SemaphoreType.DMA((4,)),
        ]
        + [packed] * 4,
        compiler_params=pltpu.CompilerParams(
            collective_id=1, has_side_effects=True, vmem_limit_bytes=49 * 1024 * 1024
        ),
        name="update_schur",
    )(neighbours, interp)


def body(fine_blocks, fine_to_coarse, widths, pivots, neighbours):
    gx_count, yz_count = lax.axis_size("gx"), lax.axis_size("yz")
    gx_pos, yz_pos = lax.axis_index("gx"), lax.axis_index("yz")
    blocks_dev = fine_blocks.shape[0]
    clusters = blocks_dev // 2
    grouped = lax.dynamic_index_in_dim(
        fine_to_coarse.reshape(gx_count, yz_count, blocks_dev), gx_pos, 0, keepdims=False
    )
    owner, local = grouped // clusters - gx_pos * yz_count, grouped % clusters
    target = lax.dynamic_index_in_dim(owner, yz_pos, 0, keepdims=False)
    mine = (owner == yz_pos)[None] & (local[None] == jnp.arange(clusters, dtype=jnp.int32)[:, None, None])
    peer = jnp.arange(yz_count, dtype=jnp.int32)[None, :, None]
    first = jnp.min(jnp.where(mine, peer, yz_count - 1), axis=(1, 2))
    second = jnp.max(jnp.where(mine, peer, 0), axis=(1, 2))
    goes = target[None, :] == jnp.arange(yz_count, dtype=jnp.int32)[:, None]
    numbers = jnp.stack([jnp.arange(blocks_dev, dtype=jnp.int32), widths])
    slots = jnp.sum(jnp.where(goes[None], numbers[:, None, :], 0), axis=2)
    interp = solve(exchange_gram(fine_blocks, slots, jnp.stack([first, second]), pivots))
    return interp, schur_of(interp, neighbours)


def solution(mesh):
    split = ("gx", "yz")
    return jax.shard_map(
        body,
        mesh=mesh,
        in_specs=(P(split, None, None), P(), P(split), P(split, None), P(split, None)),
        out_specs=(P(split, None, None), P(split, None, None)),
        check_vma=False,
    )
```
